128 devices in a mesh: dp: 32 (over y_hi, x, z), head: 4 (over y_lo, core).
Axes of the slice: x: 4, y: 4 (y_hi: 2, y_lo: 2; y = y_hi * 2 + y_lo), z: 4, core: 2. Of those that a mesh axis runs over, the one named last changes fastest.
Arguments:
- residual: bfloat16 [128, 4096], P('dp', 'head'), may hold values from -6 to 6
- query: bfloat16 [128, 32, 128], P('dp', 'head'), may hold values from -4.5 to 4.5
- fresh_token_keys: bfloat16 [128, 8, 128], P('dp', 'head'), may hold values from -4.5 to 4.5
- value_new: bfloat16 [128, 8, 128], P('dp', 'head'), may hold values from -24 to 24
- key_cache: bfloat16 [128, 8, 2048, 128], P('dp', 'head'), may hold values from -6 to 6
- value_cache: bfloat16 [128, 8, 2048, 128], P('dp', 'head'), may hold values from -6 to 6
- lengths: int32 [128], P('dp'), may hold values from 1024 to 2048, as said below
- pages: int32 [128, 8, 64], P('dp', 'head'), may hold values from 0 to 127, as said below
- w_out: bfloat16 [4096, 4096], P('head', 'dp'), may hold values from -0.75 to 0.75
- norm_gain: float32 [4096], P('head'), may hold values from 0.5 to 1.5
- expert_ids: int32 [128, 2], P('dp'), may hold values from 0 to 7, all different within a row; in each aligned block of 4 rows (0 to 3, 4 to 7, ...) at most 2 rows name the same one
- gate_weights: float32 [128, 2], P('dp'), may hold values from 0.1 to 1
- w_in: bfloat16 [32, 2, 4096, 1792], P('dp', None, None, 'head'), may hold values from -0.09375 to 0.09375
- w_down: bfloat16 [32, 1792, 4096], P('dp', 'head'), may hold values from -0.0625 to 0.0625
Outputs:
- layer_out: bfloat16 [128, 4096], P('dp', 'head')
The draws below stay inside these ranges and needn't reach their ends.
Inputs may be any that keep to these rules, and one draw needn't show every extreme that they name: `lengths`: each request's length; some request has exactly 2048 and some exactly 1024. `pages`: for each request and key head, 64 distinct page numbers, all below ceil(length / 16), always including the page that holds the request's last cached token; in no fixed order. `expert_ids`: per token 2 distinct experts; among the 4 tokens of one dp index no expert is named more than 2 times.
All inputs are finite; a program needn't handle non-finite values.
Results may differ from the reference program's by a relative error of at most 0.012.
Values may be sent and summed in bfloat16 or wider, within the bound.
A program may use at most 64 MiB of HBM per device.

```python
import math
import jax
import jax.numpy as jnp
import numpy as np
from jax import lax

D = 4096
HEADS = 32
KV_HEADS = 8
HD = 128
EXPERTS = 8
TOP = 2
FF = 7168
PAGE = 16
SEL = 64
B_DEV = 4
LEN = 2048
BATCH = 128
PAGES = 128
GROUP = 4
MOST = 2


def draw_query(key, part):
    shape = (BATCH, HEADS, HD)
    base = jax.random.truncated_normal(jax.random.fold_in(key, 1), -4.5, 4.5, shape, jnp.float32)
    return base.astype(jnp.bfloat16)


def draw_fresh_token_keys(key, part):
    shape = (BATCH, KV_HEADS, HD)
    base = 2.0 * jax.random.truncated_normal(jax.random.fold_in(key, 2), -2.25, 2.25, shape, jnp.float32)
    return base.astype(jnp.bfloat16)


def page_plan(key):
    plan_key = jax.random.fold_in(key, 11)
    length_key, end_key, shift_key, score_key = jax.random.split(plan_key, 4)
    lengths = jax.random.randint(length_key, (BATCH,), SEL * PAGE, LEN + 1, dtype=jnp.int32)
    first_end = jax.random.randint(end_key, (), 0, BATCH, dtype=jnp.int32)
    offset_scores = jax.random.randint(shift_key, (), 0, BATCH - 1, dtype=jnp.int32)
    second_end = (first_end + 1 + offset_scores) % BATCH
    lengths = lengths.at[first_end].set(LEN).at[second_end].set(SEL * PAGE)
    used_pages = (lengths + PAGE - 1) // PAGE
    page_num = jnp.arange(PAGES, dtype=jnp.int32)[None, None, :]
    scores = jax.random.randint(score_key, (BATCH, KV_HEADS, PAGES), 0, 1 << 20, dtype=jnp.int32) * PAGES + page_num
    scores = jnp.where(page_num == used_pages[:, None, None] - 1, 1 << 30, scores)
    scores = jnp.where(page_num >= used_pages[:, None, None], -1, scores)
    chosen = jax.lax.top_k(scores, SEL)[1].astype(jnp.int32)
    return (lengths, chosen)


def draw_lengths(key, part):
    return page_plan(key)[0]


def draw_pages(key, part):
    return page_plan(key)[1]


def steps_of(own_key, shape, cuts, low, top_value):
    gain, own = 1.0, jax.random.fold_in(own_key, 6)
    for dim, parts in cuts:
        steps = jnp.exp(jax.random.uniform(jax.random.fold_in(own, dim), (parts,), jnp.float32, low / len(cuts), top_value / len(cuts)))
        gain = gain * jnp.repeat(steps, shape[dim] // parts).reshape([-1 if axis == dim else 1 for axis in range(len(shape))])
    return gain


def deal_out(rng, own, number, rows, amount, top, reach, skew):
    sequence = jax.random.permutation(rng, amount)
    packed, usual = shares(amount, rows * top, reach, skew, True), shares(amount, rows * top, reach, skew, False)
    places = jnp.arange(amount)

    def named(sizes, offset_by):
        used = int((sizes > 0).sum())
        fixed = max(1, used // 4)
        passed = fixed + (places - fixed + offset_by * (used - fixed)) % max(1, amount - fixed)
        return jnp.zeros((amount,), jnp.int32).at[sequence[jnp.where(places < fixed, places, passed)]].set(jnp.asarray(sizes, jnp.int32))

    sizes = jnp.where(number % 4 == 0, named(packed, number // 4), named(usual, number - number // 4 - 1))
    mixed = jax.random.permutation(jax.random.fold_in(own, 3), amount)
    source_of, taker = mixed[0:amount // 2 * 2:2], mixed[1:amount // 2 * 2:2]
    margin = jnp.minimum(sizes[source_of] - 1, reach - sizes[taker]) // 2
    margin = jnp.where((source_of == sequence[0]) | (taker == sequence[0]) | (sizes[taker] == 0), 0, jnp.maximum(margin, 0))
    passed = jax.random.randint(jax.random.fold_in(own, 4), (amount // 2,), 0, 1 << 20) % (margin + 1)
    sizes = sizes.at[source_of].add(-passed).at[taker].add(passed)
    items = jnp.searchsorted(jnp.cumsum(sizes), jnp.arange(rows * top), side="right").astype(jnp.int32)
    listing = items.reshape(top, rows).T
    listing = listing[jax.random.permutation(jax.random.fold_in(own, 1), rows)]
    offset_by = jax.random.randint(jax.random.fold_in(own, 2), (rows, 1), 0, top)
    return jnp.take_along_axis(listing, (jnp.arange(top)[None, :] + offset_by) % top, axis=1)


def shares(count, total, reach, slope, full):
    weights = [(1 << 20) // math.isqrt(rank ** slope) + 1 for rank in range(1, count + 1)]
    largest = reach if full else min(reach, max(-(-total // count), total * weights[0] // sum(weights)))
    least = 1 if total - largest >= count - 1 else 0
    given, surplus = [largest] + [least] * (count - 1), total - largest - least * (count - 1)
    while surplus > 0:
        free = [i for i in range(1, count) if given[i] < largest] or [i for i in range(1, count) if given[i] < reach]
        whole, remaining = sum([weights[i] for i in free]), surplus
        for i in free:
            addition = min(reach - given[i], max(1, remaining * weights[i] // whole), surplus)
            given[i] = given[i] + addition
            surplus = surplus - addition
    return np.array(given)


def noise(key, shape, spread, bound, cuts=(), held_as=jnp.bfloat16):
    drawn = spread * jax.random.normal(key, shape, jnp.float32)
    if cuts:
        drawn = drawn * steps_of(key, shape, cuts, -0.22, 0.18)
    return jnp.clip(drawn, -bound, bound).astype(held_as)


def setup_inputs(seed: int = 0) -> dict:
    key_list = jax.random.split(jax.random.key(seed), 15)
    residual = noise(key_list[0], (BATCH, D), 1.0, 6.0, ((0, 32), (1, 4)))
    query = draw_query(jax.random.fold_in(key_list[14], 71), 0)
    fresh_token_keys = draw_fresh_token_keys(jax.random.fold_in(key_list[14], 71), 0)
    value_new = noise(key_list[3], (BATCH, KV_HEADS, HD), 4.0, 24.0, ((0, 32), (1, 4)))
    key_cache = noise(key_list[4], (BATCH, KV_HEADS, LEN, HD), 1.0, 6.0, ((0, 32), (1, 4)))
    value_cache = noise(key_list[5], (BATCH, KV_HEADS, LEN, HD), 1.0, 6.0, ((0, 32), (1, 4)))
    lengths = draw_lengths(jax.random.fold_in(key_list[14], 71), 0)
    pages = draw_pages(jax.random.fold_in(key_list[14], 71), 0)
    w_out = noise(key_list[8], (HEADS * HD, D), 64 ** -0.5, 0.75, ((0, 4), (1, 32)))
    norm_gain = jnp.clip(1.0 + 0.1 * jax.random.normal(key_list[9], (D,), jnp.float32), 0.5, 1.5)
    expert_ids_keys = jax.random.split(jax.random.fold_in(key_list[10], 1), BATCH // B_DEV)
    expert_ids_turns = jax.random.permutation(jax.random.fold_in(key_list[10], 3), BATCH // B_DEV)
    expert_ids = jax.vmap(lambda own, number: deal_out(jax.random.fold_in(key_list[10], 2), own, number, B_DEV, EXPERTS, TOP, MOST, 2))(expert_ids_keys, expert_ids_turns).reshape((BATCH, TOP))
    gate_weights = jnp.clip(0.1 + 0.9 * jax.random.uniform(key_list[11], (BATCH, TOP), jnp.float32) ** steps_of(key_list[11], (BATCH, TOP), ((0, 32),), -0.2, 0.2), 0.1, 1.0)
    w_in = noise(key_list[12], (EXPERTS * GROUP, 2, D, FF // GROUP), D ** -0.5, 0.09375, ((0, 32), (3, 4)))
    w_down = noise(key_list[13], (EXPERTS * GROUP, FF // GROUP, D), FF ** -0.5, 0.0625, ((0, 32), (1, 4)))
    return {"residual": residual, "query": query, "fresh_token_keys": fresh_token_keys, "value_new": value_new, "key_cache": key_cache, "value_cache": value_cache, "lengths": lengths, "pages": pages, "w_out": w_out, "norm_gain": norm_gain, "expert_ids": expert_ids, "gate_weights": gate_weights, "w_in": w_in, "w_down": w_down}


EPSILON = 1e-05

def attend(request):
    query, fresh_token_keys, value_new, key_cache, value_cache, length, page_list = request
    offsets = jnp.arange(PAGE, dtype=jnp.int32)
    positions = (page_list[:, :, None] * PAGE + offsets[None, None, :]).reshape(KV_HEADS, SEL * PAGE).astype(jnp.int32)
    sel_keys = jnp.take_along_axis(key_cache, positions[:, :, None], axis=1).astype(jnp.float32)
    sel_values = jnp.take_along_axis(value_cache, positions[:, :, None], axis=1).astype(jnp.float32)
    grouped_rows = query.reshape(KV_HEADS, HEADS // KV_HEADS, HD).astype(jnp.float32)
    score_scale = HD ** (-0.5)
    scores = jnp.einsum('kgd,ksd->kgs', grouped_rows, sel_keys) * score_scale
    own_score = jnp.einsum('kgd,kd->kg', grouped_rows, fresh_token_keys.astype(jnp.float32)) * score_scale
    in_range = (positions < length)[:, None, :]
    masked = jnp.where(in_range, scores, -1e+30)
    row_top = jnp.maximum(lax.optimization_barrier(jnp.max(masked, axis=-1)), own_score)
    expo = jnp.where(in_range, jnp.exp(scores - row_top[..., None]), 0.0)
    own_expo = jnp.exp(own_score - row_top)
    denominator = lax.optimization_barrier(jnp.sum(expo, axis=-1)) + own_expo
    weights = (expo / denominator[..., None]).astype(jnp.bfloat16)
    own_weight = (own_expo / denominator).astype(jnp.bfloat16)
    attended = jnp.einsum('kgs,ksd->kgd', weights.astype(jnp.float32), sel_values)
    attended = attended + own_weight.astype(jnp.float32)[..., None] * value_new.astype(jnp.float32)[:, None, :]
    return attended.reshape(HEADS * HD).astype(jnp.bfloat16)

def reference(residual, query, fresh_token_keys, value_new, key_cache, value_cache, lengths, pages, w_out, norm_gain, expert_ids, gate_weights, w_in, w_down):
    attn_rows = lax.map(attend, (query, fresh_token_keys, value_new, key_cache, value_cache, lengths, pages))
    stream = residual.astype(jnp.float32) + jnp.dot(attn_rows, w_out, preferred_element_type=jnp.float32)
    square_mean_value = lax.optimization_barrier(jnp.mean(stream * stream, axis=-1))
    normed = (stream * lax.rsqrt(square_mean_value + EPSILON)[:, None] * norm_gain[None, :]).astype(jnp.bfloat16)
    expert_range = jnp.arange(EXPERTS, dtype=jnp.int32)
    weight_factor = lax.optimization_barrier(jnp.sum(jnp.where(expert_ids[:, :, None] == expert_range[None, None, :], gate_weights[:, :, None], 0.0), axis=1))

    def add_expert(carry, expert):
        expert_out = jnp.zeros((BATCH, D), jnp.float32)
        for slab_part in range(GROUP):
            slab = (expert * GROUP + slab_part).astype(jnp.int32)
            pair = lax.dynamic_index_in_dim(w_in, slab, 0, keepdims=False)
            gate_act = jnp.dot(normed, pair[0], preferred_element_type=jnp.float32)
            up_act = jnp.dot(normed, pair[1], preferred_element_type=jnp.float32)
            hidden = (jax.nn.silu(gate_act) * up_act).astype(jnp.bfloat16)
            down = lax.dynamic_index_in_dim(w_down, slab, 0, keepdims=False)
            expert_out = expert_out + jnp.dot(hidden, down, preferred_element_type=jnp.float32)
        column = lax.dynamic_index_in_dim(weight_factor, expert, 1, keepdims=False)
        return (carry + column[:, None] * expert_out, None)
    mixture, unused = lax.scan(add_expert, jnp.zeros((BATCH, D), jnp.float32), expert_range)
    return (stream + mixture).astype(jnp.bfloat16)
```

```python
import functools

import jax
import jax.numpy as jnp
from jax import lax
from jax.experimental import pallas as pl
from jax.experimental.pallas import tpu as pltpu
from jax.sharding import PartitionSpec as P

EXPERTS = 8
PAGE = 16
EPSILON = 1e-05
F32 = jnp.float32
BF16 = jnp.bfloat16
I32 = jnp.int32
MESH = pl.DeviceIdType.MESH


def whole_wait(ref, sem):
    pltpu.make_async_copy(ref, ref, sem).wait()


def layer(
    ids_ref,
    gates_ref,
    len_ref,
    residual_ref,
    query_ref,
    fresh_ref,
    vnew_ref,
    pages_ref,
    gain_ref,
    key_hbm,
    value_hbm,
    wout_hbm,
    win_hbm,
    wdown_hbm,
    out_ref,
    key_buf,
    value_buf,
    wout_buf,
    win_buf,
    wdown_buf,
    attn_buf,
    recv_a,
    rows_f,
    msg_buf,
    recv_m,
    recv_g,
    part_buf,
    recv_r,
    stream_buf,
    sel_buf,
    recv_b,
    recv_s,
    x_buf,
    slab_f,
    slab_b,
    recv_c,
    mix_f,
    kv_sem,
    w_sem,
    send_sem,
    recv_sem,
):
    d = lax.axis_index("dp")
    h = lax.axis_index("head")
    me = d * 4 + h

    def device(index):
        return (index // 4, lax.rem(index, 4))

    for b in range(4):
        pltpu.make_async_copy(key_hbm.at[b], key_buf.at[b], kv_sem.at[0, b]).start()
        pltpu.make_async_copy(value_hbm.at[b], value_buf.at[b], kv_sem.at[1, b]).start()
    pltpu.make_async_copy(wout_hbm, wout_buf, w_sem.at[0]).start()
    pltpu.make_async_copy(win_hbm.at[0], win_buf, w_sem.at[1]).start()
    pltpu.make_async_copy(wdown_hbm.at[0], wdown_buf, w_sem.at[2]).start()

    barrier = pltpu.get_barrier_semaphore()

    def greet(i, carry):
        pl.semaphore_signal(
            barrier, inc=1, device_id=device(lax.rem(me + i, 128)), device_id_type=MESH
        )
        return carry

    lax.fori_loop(1, 128, greet, 0)

    ids = [ids_ref[t, j] for t in range(4) for j in range(2)]
    slots = []
    for a in range(8):
        earlier = jnp.int32(0)
        for c in range(a):
            earlier = earlier + (ids[c] == ids[a]).astype(I32)
        slots.append(earlier)
    block = lax.rem(d, 8)

    lane = lax.broadcasted_iota(I32, (8, 128), 1)
    row8 = lax.broadcasted_iota(I32, (8, 128), 0)
    target = jnp.zeros((8, 128), I32)
    for t in range(4):
        for j in range(2):
            a = t * 2 + j
            value = ids[a] * 16 + block * 2 + slots[a]
            target = jnp.where((row8 == 4 + j) & (lane == block * 4 + t), value, target)
    target = target.astype(F32)
    for j in range(8):
        res = residual_ref[:, j * 128 : (j + 1) * 128].astype(F32)
        both = jnp.concatenate([res, jnp.zeros((4, 128), F32)], axis=0)
        msg_buf[j] = (both + target).astype(BF16)

    head_lane = lax.broadcasted_iota(I32, (128, 128), 1)
    page_row = lax.broadcasted_iota(I32, (128, 64), 0)
    chosen = jnp.zeros((128, 128), F32)
    for b in range(4):
        for k in range(2):
            hit = (pages_ref[b, k : k + 1, :] == page_row).astype(F32)
            column = jnp.sum(hit, axis=1, keepdims=True)
            chosen = jnp.where((head_lane >> 2) == b * 2 + k, column, chosen)
    chosen_rows = chosen.T[:32, :].astype(BF16)
    spread = (
        (lax.broadcasted_iota(I32, (128, 2048), 1) >> 4)
        == lax.broadcasted_iota(I32, (128, 2048), 0)
    ).astype(F32).astype(BF16)
    mask = jnp.dot(chosen_rows, spread, preferred_element_type=F32)

    position = lax.broadcasted_iota(I32, (8, 2048), 1)
    top_rows = lax.broadcasted_iota(I32, (8, 1), 0) < 4
    scale = 128.0 ** (-0.5)
    nt = (((1,), (1,)), ((), ()))
    for b in range(4):
        q = query_ref[b]
        qf = q.astype(F32)
        fresh = jnp.where(
            top_rows, fresh_ref[b, 0:1, :].astype(F32), fresh_ref[b, 1:2, :].astype(F32)
        )
        own = jnp.sum(qf * fresh, axis=1, keepdims=True) * scale
        live = (mask[b * 8 : (b + 1) * 8] > 0.5) & (position < len_ref[b])
        pltpu.make_async_copy(key_hbm.at[b], key_buf.at[b], kv_sem.at[0, b]).wait()
        s0 = lax.dot_general(q, key_buf[b, 0], nt, preferred_element_type=F32)
        s1 = lax.dot_general(q, key_buf[b, 1], nt, preferred_element_type=F32)
        scores = jnp.where(top_rows, s0, s1) * scale
        masked = jnp.where(live, scores, -1e30)
        top = jnp.maximum(jnp.max(masked, axis=1, keepdims=True), own)
        expo = jnp.where(live, jnp.exp(scores - top), 0.0)
        own_expo = jnp.exp(own - top)
        total = jnp.sum(expo, axis=1, keepdims=True) + own_expo
        weights = (expo / total).astype(BF16)
        own_weight = (own_expo / total).astype(BF16).astype(F32)
        pltpu.make_async_copy(value_hbm.at[b], value_buf.at[b], kv_sem.at[1, b]).wait()
        a0 = jnp.dot(weights, value_buf[b, 0], preferred_element_type=F32)
        a1 = jnp.dot(weights, value_buf[b, 1], preferred_element_type=F32)
        new = jnp.where(
            top_rows, vnew_ref[b, 0:1, :].astype(F32), vnew_ref[b, 1:2, :].astype(F32)
        )
        attn_buf[b * 8 : (b + 1) * 8, :] = (
            jnp.where(top_rows, a0, a1) + own_weight * new
        ).astype(BF16)

    pl.semaphore_wait(barrier, 127)

    def send_rows(i, carry):
        to = lax.rem(d + i, 32)
        pltpu.make_async_remote_copy(
            attn_buf, recv_a.at[d], send_sem.at[0], recv_sem.at[0], (to, h), MESH
        ).start()
        return carry

    lax.fori_loop(1, 32, send_rows, 0)
    pltpu.make_async_copy(attn_buf, recv_a.at[d], recv_sem.at[0]).start()

    quarter = d // 8

    def send_message(j, carry):
        to = h * 8 + j
        here = (to == d) & (quarter == h)

        @pl.when(here)
        def _():
            pltpu.make_async_copy(msg_buf.at[j], recv_m.at[block], recv_sem.at[1]).start()

        @pl.when(jnp.logical_not(here))
        def _():
            pltpu.make_async_remote_copy(
                msg_buf.at[j],
                recv_m.at[block],
                send_sem.at[1],
                recv_sem.at[1],
                (to, quarter),
                MESH,
            ).start()

        return carry

    lax.fori_loop(0, 8, send_message, 0)
    for i in range(1, 4):
        pltpu.make_async_remote_copy(
            gain_ref, recv_g.at[h], send_sem.at[2], recv_sem.at[2], (d, lax.rem(h + i, 4)), MESH
        ).start()
    pltpu.make_async_copy(gain_ref, recv_g.at[h], recv_sem.at[2]).start()

    whole_wait(recv_m, recv_sem.at[1])
    messages = recv_m[...].astype(F32).reshape(64, 128).astype(BF16)
    pick_row = lax.broadcasted_iota(I32, (40, 64), 0)
    pick_col = lax.broadcasted_iota(I32, (40, 64), 1)
    pick = (
        ((pick_row < 32) & (pick_col == (pick_row >> 2) * 8 + (pick_row & 3)))
        | ((pick_row == 32) & ((pick_col & 7) == 4))
        | ((pick_row == 33) & ((pick_col & 7) == 5))
    )
    picked = jnp.dot(pick.astype(F32).astype(BF16), messages, preferred_element_type=F32)
    residual = picked[:32]
    slot_row = lax.broadcasted_iota(I32, (128, 128), 0).astype(F32)
    select = ((slot_row == picked[32:33]) | (slot_row == picked[33:34])).astype(F32)
    select = select[:, :32].astype(BF16)
    pltpu.make_async_copy(wout_hbm, wout_buf, w_sem.at[0]).wait()

    whole_wait(recv_a, recv_sem.at[0])
    rows_f[...] = recv_a[...].astype(F32).reshape(1024, 128)
    columns = jnp.zeros((128, 128), F32)
    for n in range(4):
        pair = jnp.concatenate(
            [rows_f[pl.ds(n * 2 + m, 128, stride=8), :] for m in range(2)], axis=1
        ).astype(BF16)
        columns = columns + jnp.dot(
            pair, wout_buf[n * 256 : (n + 1) * 256, :], preferred_element_type=F32
        )
    part_buf[...] = columns.astype(BF16).reshape(4, 32, 128)

    for i in range(1, 4):
        to = lax.rem(h + i, 4)
        pltpu.make_async_remote_copy(
            part_buf.at[to], recv_r.at[h], send_sem.at[3], recv_sem.at[3], (d, to), MESH
        ).start()
    pltpu.make_async_copy(part_buf.at[h], recv_r.at[h], recv_sem.at[3]).start()
    whole_wait(recv_r, recv_sem.at[3])
    stream = residual
    for i in range(4):
        stream = stream + recv_r[i].astype(F32)
    stream_buf[...] = stream.reshape(4, 8, 128)
    sel_buf[...] = (
        jnp.dot(select, stream.astype(BF16), preferred_element_type=F32)
        .astype(BF16)
        .reshape(8, 16, 128)
    )

    def send_slots(i, carry):
        to = lax.rem(me + i, 128)
        pltpu.make_async_remote_copy(
            sel_buf.at[to // 16],
            recv_b.at[me],
            send_sem.at[4],
            recv_sem.at[4],
            device(to),
            MESH,
        ).start()
        return carry

    lax.fori_loop(1, 128, send_slots, 0)
    pltpu.make_async_copy(sel_buf.at[me // 16], recv_b.at[me], recv_sem.at[4]).start()

    def send_stream(b, carry):
        to = h * 8 + b
        here = (to == d) & (quarter == h)

        @pl.when(here)
        def _():
            pltpu.make_async_copy(
                stream_buf.at[b // 2], recv_s.at[block], recv_sem.at[5]
            ).start()

        @pl.when(jnp.logical_not(here))
        def _():
            pltpu.make_async_remote_copy(
                stream_buf.at[b // 2],
                recv_s.at[block],
                send_sem.at[5],
                recv_sem.at[5],
                (to, quarter),
                MESH,
            ).start()

        return carry

    lax.fori_loop(0, 8, send_stream, 0)

    pltpu.make_async_copy(win_hbm.at[0], win_buf, w_sem.at[1]).wait()
    pltpu.make_async_copy(wdown_hbm.at[0], wdown_buf, w_sem.at[2]).wait()
    whole_wait(recv_g, recv_sem.at[2])
    whole_wait(recv_b, recv_sem.at[4])
    squares = jnp.zeros((64, 128), F32)
    for n in range(32):
        x = recv_b[n * 4 : (n + 1) * 4].reshape(64, 128).astype(F32)
        squares = squares + x * x
        x_buf[:, n * 128 : (n + 1) * 128] = (
            x * recv_g[n // 8, n % 8 : n % 8 + 1, :]
        ).astype(BF16)
    inverse = lax.rsqrt(jnp.sum(squares, axis=1, keepdims=True) * (1.0 / 4096.0) + EPSILON)
    gate = jnp.dot(x_buf[...], win_buf[0], preferred_element_type=F32) * inverse
    up = jnp.dot(x_buf[...], win_buf[1], preferred_element_type=F32) * inverse
    hidden = (gate * jax.nn.sigmoid(gate) * up).astype(BF16)
    for n in range(16):
        slab = jnp.dot(
            hidden, wdown_buf[:, n * 256 : (n + 1) * 256], preferred_element_type=F32
        )
        for m in range(2):
            j = (n * 2 + m) % 8
            slab_f[n // 4, pl.ds(j, 64, stride=8), :] = slab[:, m * 128 : (m + 1) * 128]
    slab_b[...] = slab_f[...].astype(BF16).reshape(4, 32, 16, 128)

    def send_back(i, carry):
        to = lax.rem(me + i, 128)
        pltpu.make_async_remote_copy(
            slab_b.at[lax.rem(to, 4), to // 4],
            recv_c.at[me],
            send_sem.at[6],
            recv_sem.at[6],
            device(to),
            MESH,
        ).start()
        return carry

    lax.fori_loop(1, 128, send_back, 0)
    pltpu.make_async_copy(slab_b.at[h, d], recv_c.at[me], recv_sem.at[6]).start()

    slot16 = lax.broadcasted_iota(I32, (16, 128), 0)
    factors = []
    for t in range(4):
        factor = jnp.zeros((16, 128), F32)
        for j in range(2):
            a = t * 2 + j
            factor = factor + jnp.where(slot16 == ids[a] * 2 + slots[a], gates_ref[t, j], 0.0)
        factors.append(factor)
    odd = lax.rem(d, 2) == 1

    whole_wait(recv_s, recv_sem.at[5])
    whole_wait(recv_c, recv_sem.at[6])
    for e in range(8):
        total = recv_c[e * 16].astype(F32)
        for i in range(1, 16):
            total = total + recv_c[e * 16 + i].astype(F32)
        mix_f[e * 16 : (e + 1) * 16, :] = total
    for j in range(8):
        slot_rows = mix_f[pl.ds(j, 16, stride=8), :]
        mixed = jnp.concatenate(
            [jnp.sum(slot_rows * f, axis=0, keepdims=True) for f in factors], axis=0
        )
        own_stream = recv_s[j]
        own_stream = jnp.where(odd, own_stream[4:], own_stream[:4])
        out_ref[:, j * 128 : (j + 1) * 128] = (own_stream + mixed).astype(BF16)

    whole_wait(recv_a.at[pl.ds(0, 31)], send_sem.at[0])
    apart = (quarter != h).astype(I32)

    @pl.when(quarter == h)
    def _():
        whole_wait(recv_m.at[pl.ds(0, 7)], send_sem.at[1])
        whole_wait(recv_s.at[pl.ds(0, 7)], send_sem.at[5])

    @pl.when(quarter != h)
    def _():
        whole_wait(recv_m, send_sem.at[1])
        whole_wait(recv_s, send_sem.at[5])

    whole_wait(recv_g.at[pl.ds(0, 3)], send_sem.at[2])
    whole_wait(recv_r.at[pl.ds(0, 3)], send_sem.at[3])
    whole_wait(recv_b.at[pl.ds(0, 127)], send_sem.at[4])
    whole_wait(recv_c.at[pl.ds(0, 127)], send_sem.at[6])


def shards(
    residual,
    query,
    fresh_token_keys,
    value_new,
    key_cache,
    value_cache,
    lengths,
    pages,
    w_out,
    norm_gain,
    expert_ids,
    gate_weights,
    w_in,
    w_down,
):
    smem = pl.BlockSpec(memory_space=pltpu.SMEM)
    vmem = pl.BlockSpec(memory_space=pltpu.VMEM)
    hbm = pl.BlockSpec(memory_space=pltpu.HBM)
    return pl.pallas_call(
        layer,
        out_shape=jax.ShapeDtypeStruct((4, 1024), BF16),
        in_specs=[smem] * 3 + [vmem] * 6 + [hbm] * 5,
        out_specs=vmem,
        scratch_shapes=[
            pltpu.VMEM((4, 2, 2048, 128), BF16),
            pltpu.VMEM((4, 2, 2048, 128), BF16),
            pltpu.VMEM((1024, 128), BF16),
            pltpu.VMEM((2, 4096, 448), BF16),
            pltpu.VMEM((448, 4096), BF16),
            pltpu.VMEM((32, 128), BF16),
            pltpu.VMEM((32, 32, 128), BF16),
            pltpu.VMEM((1024, 128), F32),
            pltpu.VMEM((8, 8, 128), BF16),
            pltpu.VMEM((8, 8, 128), BF16),
            pltpu.VMEM((4, 8, 128), F32),
            pltpu.VMEM((4, 32, 128), BF16),
            pltpu.VMEM((4, 32, 128), BF16),
            pltpu.VMEM((4, 8, 128), F32),
            pltpu.VMEM((8, 16, 128), BF16),
            pltpu.VMEM((128, 16, 128), BF16),
            pltpu.VMEM((8, 8, 128), F32),
            pltpu.VMEM((64, 4096), BF16),
            pltpu.VMEM((4, 512, 128), F32),
            pltpu.VMEM((4, 32, 16, 128), BF16),
            pltpu.VMEM((128, 16, 128), BF16),
            pltpu.VMEM((128, 128), F32),
            pltpu.SemaphoreType.DMA((2, 4)),
            pltpu.SemaphoreType.DMA((3,)),
            pltpu.SemaphoreType.DMA((7,)),
            pltpu.SemaphoreType.DMA((7,)),
        ],
        compiler_params=pltpu.CompilerParams(
            collective_id=0, has_side_effects=True, vmem_limit_bytes=60 * 1024 * 1024
        ),
        name="layer",
    )(
        expert_ids,
        gate_weights,
        lengths,
        residual,
        query,
        fresh_token_keys,
        value_new,
        pages,
        norm_gain.reshape(8, 128),
        key_cache,
        value_cache,
        w_out,
        w_in,
        w_down,
    )


def solution(mesh):
    in_specs = (
        P("dp", "head"),
        P("dp", "head", None),
        P("dp", "head", None),
        P("dp", "head", None),
        P("dp", "head", None, None),
        P("dp", "head", None, None),
        P("dp"),
        P("dp", "head", None),
        P("head", "dp"),
        P("head"),
        P("dp", None),
        P("dp", None),
        P("dp", None, None, "head"),
        P("dp", "head", None),
    )
    out_specs = P("dp", "head")
    return jax.shard_map(shards, mesh=mesh, in_specs=in_specs, out_specs=out_specs, check_vma=False)
```

```python
import functools

import jax
import jax.numpy as jnp
from jax import lax
from jax.experimental import pallas as pl
from jax.experimental.pallas import tpu as pltpu
from jax.sharding import PartitionSpec as P

EXPERTS = 8
PAGE = 16
EPSILON = 1e-05
F32 = jnp.float32
BF16 = jnp.bfloat16
I32 = jnp.int32
MESH = pl.DeviceIdType.MESH


def whole_wait(ref, sem):
    pltpu.make_async_copy(ref, ref, sem).wait()


def layer(
    ids_ref,
    gates_ref,
    len_ref,
    residual_ref,
    query_ref,
    fresh_ref,
    vnew_ref,
    pages_ref,
    gain_ref,
    key_hbm,
    value_hbm,
    wout_hbm,
    win_hbm,
    wdown_hbm,
    out_ref,
    key_buf,
    value_buf,
    wout_buf,
    win_buf,
    wdown_buf,
    attn_buf,
    recv_a,
    rows_f,
    msg_buf,
    recv_m,
    recv_g,
    part_buf,
    recv_r,
    stream_buf,
    sel_buf,
    recv_b,
    recv_s,
    x_buf,
    slab_f,
    slab_b,
    recv_c,
    mix_f,
    kv_sem,
    w_sem,
    send_sem,
    recv_sem,
):
    d = lax.axis_index("dp")
    h = lax.axis_index("head")
    me = d * 4 + h

    def device(index):
        return (index // 4, lax.rem(index, 4))

    for b in range(4):
        pltpu.make_async_copy(key_hbm.at[b], key_buf.at[b], kv_sem.at[0, b]).start()
        pltpu.make_async_copy(value_hbm.at[b], value_buf.at[b], kv_sem.at[1, b]).start()
    pltpu.make_async_copy(wout_hbm, wout_buf, w_sem.at[0]).start()
    pltpu.make_async_copy(win_hbm.at[0], win_buf, w_sem.at[1]).start()
    pltpu.make_async_copy(wdown_hbm.at[0], wdown_buf, w_sem.at[2]).start()

    barrier = pltpu.get_barrier_semaphore()

    def greet(i, carry):
        pl.semaphore_signal(
            barrier, inc=1, device_id=device(lax.rem(me + i, 128)), device_id_type=MESH
        )
        return carry

    lax.fori_loop(1, 128, greet, 0)

    ids = [ids_ref[j, t] for t in range(4) for j in range(2)]
    slots = []
    for a in range(8):
        earlier = jnp.int32(0)
        for c in range(a):
            earlier = earlier + (ids[c] == ids[a]).astype(I32)
        slots.append(earlier)
    block = lax.rem(d, 8)

    lane = lax.broadcasted_iota(I32, (8, 128), 1)
    row8 = lax.broadcasted_iota(I32, (8, 128), 0)
    target = jnp.zeros((8, 128), I32)
    for t in range(4):
        for j in range(2):
            a = t * 2 + j
            value = ids[a] * 16 + block * 2 + slots[a]
            target = jnp.where((row8 == 4 + j) & (lane == block * 4 + t), value, target)
    target = target.astype(F32)
    for j in range(8):
        res = residual_ref[:, j * 128 : (j + 1) * 128].astype(F32)
        both = jnp.concatenate([res, jnp.zeros((4, 128), F32)], axis=0)
        msg_buf[j] = (both + target).astype(BF16)

    head_lane = lax.broadcasted_iota(I32, (128, 128), 1)
    page_row = lax.broadcasted_iota(I32, (128, 64), 0)
    chosen = jnp.zeros((128, 128), F32)
    for b in range(4):
        for k in range(2):
            hit = (pages_ref[b, k : k + 1, :] == page_row).astype(F32)
            column = jnp.sum(hit, axis=1, keepdims=True)
            chosen = jnp.where((head_lane >> 2) == b * 2 + k, column, chosen)
    chosen_rows = chosen.T[:32, :].astype(BF16)
    spread = (
        (lax.broadcasted_iota(I32, (128, 2048), 1) >> 4)
        == lax.broadcasted_iota(I32, (128, 2048), 0)
    ).astype(F32).astype(BF16)
    mask = jnp.dot(chosen_rows, spread, preferred_element_type=F32)

    position = lax.broadcasted_iota(I32, (8, 2048), 1)
    top_rows = lax.broadcasted_iota(I32, (8, 1), 0) < 4
    scale = 128.0 ** (-0.5)
    nt = (((1,), (1,)), ((), ()))
    for b in range(4):
        q = query_ref[b]
        qf = q.astype(F32)
        fresh = jnp.where(
            top_rows, fresh_ref[b, 0:1, :].astype(F32), fresh_ref[b, 1:2, :].astype(F32)
        )
        own = jnp.sum(qf * fresh, axis=1, keepdims=True) * scale
        live = (mask[b * 8 : (b + 1) * 8] > 0.5) & (position < len_ref[b])
        pltpu.make_async_copy(key_hbm.at[b], key_buf.at[b], kv_sem.at[0, b]).wait()
        s0 = lax.dot_general(q, key_buf[b, 0], nt, preferred_element_type=F32)
        s1 = lax.dot_general(q, key_buf[b, 1], nt, preferred_element_type=F32)
        scores = jnp.where(top_rows, s0, s1) * scale
        masked = jnp.where(live, scores, -1e30)
        top = jnp.maximum(jnp.max(masked, axis=1, keepdims=True), own)
        expo = jnp.where(live, jnp.exp(scores - top), 0.0)
        own_expo = jnp.exp(own - top)
        total = jnp.sum(expo, axis=1, keepdims=True) + own_expo
        weights = (expo / total).astype(BF16)
        own_weight = (own_expo / total).astype(BF16).astype(F32)
        pltpu.make_async_copy(value_hbm.at[b], value_buf.at[b], kv_sem.at[1, b]).wait()
        a0 = jnp.dot(weights, value_buf[b, 0], preferred_element_type=F32)
        a1 = jnp.dot(weights, value_buf[b, 1], preferred_element_type=F32)
        new = jnp.where(
            top_rows, vnew_ref[b, 0:1, :].astype(F32), vnew_ref[b, 1:2, :].astype(F32)
        )
        attn_buf[b * 8 : (b + 1) * 8, :] = (
            jnp.where(top_rows, a0, a1) + own_weight * new
        ).astype(BF16)

    pl.semaphore_wait(barrier, 127)

    def send_rows(i, carry):
        to = lax.rem(d + i, 32)
        pltpu.make_async_remote_copy(
            attn_buf, recv_a.at[d], send_sem.at[0], recv_sem.at[0], (to, h), MESH
        ).start()
        return carry

    lax.fori_loop(1, 32, send_rows, 0)
    pltpu.make_async_copy(attn_buf, recv_a.at[d], recv_sem.at[0]).start()

    quarter = d // 8

    def send_message(j, carry):
        to = h * 8 + j
        here = (to == d) & (quarter == h)

        @pl.when(here)
        def _():
            pltpu.make_async_copy(msg_buf.at[j], recv_m.at[block], recv_sem.at[1]).start()

        @pl.when(jnp.logical_not(here))
        def _():
            pltpu.make_async_remote_copy(
                msg_buf.at[j],
                recv_m.at[block],
                send_sem.at[1],
                recv_sem.at[1],
                (to, quarter),
                MESH,
            ).start()

        return carry

    lax.fori_loop(0, 8, send_message, 0)
    for i in range(1, 4):
        pltpu.make_async_remote_copy(
            gain_ref, recv_g.at[h], send_sem.at[2], recv_sem.at[2], (d, lax.rem(h + i, 4)), MESH
        ).start()
    pltpu.make_async_copy(gain_ref, recv_g.at[h], recv_sem.at[2]).start()

    whole_wait(recv_m, recv_sem.at[1])
    messages = recv_m[...].astype(F32).reshape(64, 128).astype(BF16)
    pick_row = lax.broadcasted_iota(I32, (40, 64), 0)
    pick_col = lax.broadcasted_iota(I32, (40, 64), 1)
    pick = (
        ((pick_row < 32) & (pick_col == (pick_row >> 2) * 8 + (pick_row & 3)))
        | ((pick_row == 32) & ((pick_col & 7) == 4))
        | ((pick_row == 33) & ((pick_col & 7) == 5))
    )
    picked = jnp.dot(pick.astype(F32).astype(BF16), messages, preferred_element_type=F32)
    residual = picked[:32]
    slot_row = lax.broadcasted_iota(I32, (128, 128), 0).astype(F32)
    select = ((slot_row == picked[32:33]) | (slot_row == picked[33:34])).astype(F32)
    select = select[:, :32].astype(BF16)
    pltpu.make_async_copy(wout_hbm, wout_buf, w_sem.at[0]).wait()

    whole_wait(recv_a, recv_sem.at[0])
    rows_f[...] = recv_a[...].astype(F32).reshape(1024, 128)
    columns = jnp.zeros((128, 128), F32)
    for n in range(4):
        pair = jnp.concatenate(
            [rows_f[pl.ds(n * 2 + m, 128, stride=8), :] for m in range(2)], axis=1
        ).astype(BF16)
        columns = columns + jnp.dot(
            pair, wout_buf[n * 256 : (n + 1) * 256, :], preferred_element_type=F32
        )
    part_buf[...] = columns.astype(BF16).reshape(4, 32, 128)

    for i in range(1, 4):
        to = lax.rem(h + i, 4)
        pltpu.make_async_remote_copy(
            part_buf.at[to], recv_r.at[h], send_sem.at[3], recv_sem.at[3], (d, to), MESH
        ).start()
    pltpu.make_async_copy(part_buf.at[h], recv_r.at[h], recv_sem.at[3]).start()
    whole_wait(recv_r, recv_sem.at[3])
    stream = residual
    for i in range(4):
        stream = stream + recv_r[i].astype(F32)
    stream_buf[...] = stream.reshape(4, 8, 128)
    sel_buf[...] = (
        jnp.dot(select, stream.astype(BF16), preferred_element_type=F32)
        .astype(BF16)
        .reshape(8, 16, 128)
    )

    def send_slots(i, carry):
        to = lax.rem(me + i, 128)
        pltpu.make_async_remote_copy(
            sel_buf.at[to // 16],
            recv_b.at[me],
            send_sem.at[4],
            recv_sem.at[4],
            device(to),
            MESH,
        ).start()
        return carry

    lax.fori_loop(1, 128, send_slots, 0)
    pltpu.make_async_copy(sel_buf.at[me // 16], recv_b.at[me], recv_sem.at[4]).start()

    def send_stream(b, carry):
        to = h * 8 + b
        here = (to == d) & (quarter == h)

        @pl.when(here)
        def _():
            pltpu.make_async_copy(
                stream_buf.at[b // 2], recv_s.at[block], recv_sem.at[5]
            ).start()

        @pl.when(jnp.logical_not(here))
        def _():
            pltpu.make_async_remote_copy(
                stream_buf.at[b // 2],
                recv_s.at[block],
                send_sem.at[5],
                recv_sem.at[5],
                (to, quarter),
                MESH,
            ).start()

        return carry

    lax.fori_loop(0, 8, send_stream, 0)

    pltpu.make_async_copy(win_hbm.at[0], win_buf, w_sem.at[1]).wait()
    pltpu.make_async_copy(wdown_hbm.at[0], wdown_buf, w_sem.at[2]).wait()
    whole_wait(recv_g, recv_sem.at[2])
    whole_wait(recv_b, recv_sem.at[4])
    squares = jnp.zeros((64, 128), F32)
    for n in range(32):
        x = recv_b[n * 4 : (n + 1) * 4].reshape(64, 128).astype(F32)
        squares = squares + x * x
        x_buf[:, n * 128 : (n + 1) * 128] = (
            x * recv_g[n // 8, n % 8 : n % 8 + 1, :]
        ).astype(BF16)
    inverse = lax.rsqrt(jnp.sum(squares, axis=1, keepdims=True) * (1.0 / 4096.0) + EPSILON)
    gate = lax.dot_general(x_buf[...], win_buf[0], nt, preferred_element_type=F32) * inverse
    up = lax.dot_general(x_buf[...], win_buf[1], nt, preferred_element_type=F32) * inverse
    hidden = (gate * jax.nn.sigmoid(gate) * up).astype(BF16)
    for n in range(16):
        slab = jnp.dot(
            hidden, wdown_buf[:, n * 256 : (n + 1) * 256], preferred_element_type=F32
        )
        for m in range(2):
            j = (n * 2 + m) % 8
            slab_f[n // 4, pl.ds(j, 64, stride=8), :] = slab[:, m * 128 : (m + 1) * 128]
    slab_b[...] = slab_f[...].astype(BF16).reshape(4, 32, 16, 128)

    def send_back(i, carry):
        to = lax.rem(me + i, 128)
        pltpu.make_async_remote_copy(
            slab_b.at[lax.rem(to, 4), to // 4],
            recv_c.at[me],
            send_sem.at[6],
            recv_sem.at[6],
            device(to),
            MESH,
        ).start()
        return carry

    lax.fori_loop(1, 128, send_back, 0)
    pltpu.make_async_copy(slab_b.at[h, d], recv_c.at[me], recv_sem.at[6]).start()

    slot16 = lax.broadcasted_iota(I32, (16, 128), 0)
    factors = []
    for t in range(4):
        factor = jnp.zeros((16, 128), F32)
        for j in range(2):
            a = t * 2 + j
            factor = factor + jnp.where(slot16 == ids[a] * 2 + slots[a], gates_ref[j, t], 0.0)
        factors.append(factor)
    odd = lax.rem(d, 2) == 1

    whole_wait(recv_s, recv_sem.at[5])
    whole_wait(recv_c, recv_sem.at[6])
    for e in range(8):
        total = recv_c[e * 16].astype(F32)
        for i in range(1, 16):
            total = total + recv_c[e * 16 + i].astype(F32)
        mix_f[e * 16 : (e + 1) * 16, :] = total
    for j in range(8):
        slot_rows = mix_f[pl.ds(j, 16, stride=8), :]
        mixed = jnp.concatenate(
            [jnp.sum(slot_rows * f, axis=0, keepdims=True) for f in factors], axis=0
        )
        own_stream = recv_s[j]
        own_stream = jnp.where(odd, own_stream[4:], own_stream[:4])
        out_ref[:, j * 128 : (j + 1) * 128] = (own_stream + mixed).astype(BF16)

    whole_wait(recv_a.at[pl.ds(0, 31)], send_sem.at[0])
    apart = (quarter != h).astype(I32)

    @pl.when(quarter == h)
    def _():
        whole_wait(recv_m.at[pl.ds(0, 7)], send_sem.at[1])
        whole_wait(recv_s.at[pl.ds(0, 7)], send_sem.at[5])

    @pl.when(quarter != h)
    def _():
        whole_wait(recv_m, send_sem.at[1])
        whole_wait(recv_s, send_sem.at[5])

    whole_wait(recv_g.at[pl.ds(0, 3)], send_sem.at[2])
    whole_wait(recv_r.at[pl.ds(0, 3)], send_sem.at[3])
    whole_wait(recv_b.at[pl.ds(0, 127)], send_sem.at[4])
    whole_wait(recv_c.at[pl.ds(0, 127)], send_sem.at[6])


def shards(
    residual,
    query,
    fresh_token_keys,
    value_new,
    key_cache,
    value_cache,
    lengths,
    pages,
    w_out,
    norm_gain,
    expert_ids,
    gate_weights,
    w_in,
    w_down,
):
    smem = pl.BlockSpec(memory_space=pltpu.SMEM)
    vmem = pl.BlockSpec(memory_space=pltpu.VMEM)
    hbm = pl.BlockSpec(memory_space=pltpu.HBM)
    return pl.pallas_call(
        layer,
        out_shape=jax.ShapeDtypeStruct((4, 1024), BF16),
        in_specs=[smem] * 3 + [vmem] * 6 + [hbm] * 5,
        out_specs=vmem,
        scratch_shapes=[
            pltpu.VMEM((4, 2, 2048, 128), BF16),
            pltpu.VMEM((4, 2, 2048, 128), BF16),
            pltpu.VMEM((1024, 128), BF16),
            pltpu.VMEM((2, 448, 4096), BF16),
            pltpu.VMEM((448, 4096), BF16),
            pltpu.VMEM((32, 128), BF16),
            pltpu.VMEM((32, 32, 128), BF16),
            pltpu.VMEM((1024, 128), F32),
            pltpu.VMEM((8, 8, 128), BF16),
            pltpu.VMEM((8, 8, 128), BF16),
            pltpu.VMEM((4, 8, 128), F32),
            pltpu.VMEM((4, 32, 128), BF16),
            pltpu.VMEM((4, 32, 128), BF16),
            pltpu.VMEM((4, 8, 128), F32),
            pltpu.VMEM((8, 16, 128), BF16),
            pltpu.VMEM((128, 16, 128), BF16),
            pltpu.VMEM((8, 8, 128), F32),
            pltpu.VMEM((64, 4096), BF16),
            pltpu.VMEM((4, 512, 128), F32),
            pltpu.VMEM((4, 32, 16, 128), BF16),
            pltpu.VMEM((128, 16, 128), BF16),
            pltpu.VMEM((128, 128), F32),
            pltpu.SemaphoreType.DMA((2, 4)),
            pltpu.SemaphoreType.DMA((3,)),
            pltpu.SemaphoreType.DMA((7,)),
            pltpu.SemaphoreType.DMA((7,)),
        ],
        compiler_params=pltpu.CompilerParams(
            collective_id=0, has_side_effects=True, vmem_limit_bytes=60 * 1024 * 1024
        ),
        name="layer",
    )(
        expert_ids.T,
        gate_weights.T,
        lengths,
        residual,
        query,
        fresh_token_keys,
        value_new,
        pages,
        norm_gain.reshape(8, 128),
        key_cache,
        value_cache,
        w_out,
        jnp.swapaxes(w_in, 2, 3),
        w_down,
    )


def solution(mesh):
    in_specs = (
        P("dp", "head"),
        P("dp", "head", None),
        P("dp", "head", None),
        P("dp", "head", None),
        P("dp", "head", None, None),
        P("dp", "head", None, None),
        P("dp"),
        P("dp", "head", None),
        P("head", "dp"),
        P("head"),
        P("dp", None),
        P("dp", None),
        P("dp", None, None, "head"),
        P("dp", "head", None),
    )
    out_specs = P("dp", "head")
    return jax.shard_map(shards, mesh=mesh, in_specs=in_specs, out_specs=out_specs, check_vma=False)
```

```python
import functools

import jax
import jax.numpy as jnp
from jax import lax
from jax.experimental import pallas as pl
from jax.experimental.pallas import tpu as pltpu
from jax.sharding import PartitionSpec as P

EXPERTS = 8
PAGE = 16
EPSILON = 1e-05
F32 = jnp.float32
BF16 = jnp.bfloat16
I32 = jnp.int32
MESH = pl.DeviceIdType.MESH
FAR = sorted(range(1, 32), key=lambda i: -(2 * (i >> 4) + (0, 1, 2, 1)[i >> 2 & 3] + (0, 1, 2, 1)[i & 3]))
ORDER = (0, 1, 2, 3)
OUT_SPACE = pl.ANY


def whole_wait(ref, sem):
    pltpu.make_async_copy(ref, ref, sem).wait()


def layer(
    ids_hbm,
    gates_hbm,
    len_hbm,
    residual_hbm,
    query_hbm,
    fresh_hbm,
    vnew_hbm,
    pages_hbm,
    gain_hbm,
    key_hbm,
    value_hbm,
    wout_hbm,
    win_hbm,
    wdown_hbm,
    out_hbm,
    ids_ref,
    gates_ref,
    len_ref,
    residual_ref,
    query_ref,
    fresh_ref,
    vnew_ref,
    pages_ref,
    gain_ref,
    out_ref,
    key_buf,
    value_buf,
    wout_buf,
    win_buf,
    wdown_buf,
    attn_buf,
    recv_a,
    rows_f,
    msg_buf,
    recv_m,
    recv_g,
    part_buf,
    recv_r,
    stream_buf,
    sel_buf,
    recv_b,
    recv_s,
    x_buf,
    slab_f,
    sib_buf,
    recv_d,
    slab_b,
    recv_c,
    mix_f,
    in_sem,
    kv_sem,
    w_sem,
    send_sem,
    recv_sem,
    group_sem,
    pass_send,
    pass_recv,
    sib_send,
    sib_recv,
):
    d = lax.axis_index("dp")
    h = lax.axis_index("head")
    y = h >> 1
    c = h & 1
    sibling = (d, h ^ 1)
    quarter = d >> 3
    block = d & 7

    barrier = pltpu.get_barrier_semaphore()

    def greet(to):
        pl.semaphore_signal(barrier, inc=1, device_id=to, device_id_type=MESH)

    small = [
        (ids_hbm, ids_ref),
        (gates_hbm, gates_ref),
        (len_hbm, len_ref),
        (pages_hbm, pages_ref),
        (query_hbm, query_ref),
        (fresh_hbm, fresh_ref),
        (residual_hbm, residual_ref),
        (vnew_hbm, vnew_ref),
        (gain_hbm, gain_ref),
    ]
    for n, (source, target) in enumerate(small):
        pltpu.make_async_copy(source, target, in_sem.at[n]).start()

    for i in FAR:
        for side in range(2):
            greet((d ^ i, side * 2 + c))
    for i in range(1, 4):
        greet((d, h ^ i))
    for j in range(8):

        @pl.when(jnp.logical_not((h * 8 + j == d) & (quarter == h)))
        def _():
            greet((h * 8 + j, quarter))

    for b in range(4):
        pltpu.make_async_copy(key_hbm.at[b], key_buf.at[b], kv_sem.at[0, b]).start()
        pltpu.make_async_copy(value_hbm.at[b], value_buf.at[b], kv_sem.at[1, b]).start()
    for n, (source, target) in enumerate(small):
        pltpu.make_async_copy(source, target, in_sem.at[n]).wait()

    ids = [ids_ref[j, t] for t in range(4) for j in range(2)]
    slots = []
    for a in range(8):
        earlier = jnp.int32(0)
        for n in range(a):
            earlier = earlier + (ids[n] == ids[a]).astype(I32)
        slots.append(earlier)
    lane = lax.broadcasted_iota(I32, (8, 128), 1)
    row8 = lax.broadcasted_iota(I32, (8, 128), 0)
    target = jnp.zeros((8, 128), I32)
    for t in range(4):
        for j in range(2):
            a = t * 2 + j
            value = ids[a] * 16 + block * 2 + slots[a]
            target = jnp.where((row8 == 4 + j) & (lane == block * 4 + t), value, target)
    target = target.astype(F32)
    for j in range(8):
        res = residual_ref[:, j * 128 : (j + 1) * 128].astype(F32)
        both = jnp.concatenate([res, jnp.zeros((4, 128), F32)], axis=0)
        msg_buf[j] = (both + target).astype(BF16)

    head_lane = lax.broadcasted_iota(I32, (128, 128), 1)
    page_row = lax.broadcasted_iota(I32, (128, 64), 0)
    chosen = jnp.zeros((128, 128), F32)
    for b in range(4):
        for k in range(2):
            hit = (pages_ref[b, k : k + 1, :] == page_row).astype(F32)
            column = jnp.sum(hit, axis=1, keepdims=True)
            chosen = jnp.where((head_lane >> 2) == b * 2 + k, column, chosen)
    chosen_rows = chosen.T[:32, :].astype(BF16)
    spread = (
        (lax.broadcasted_iota(I32, (128, 2048), 1) >> 4)
        == lax.broadcasted_iota(I32, (128, 2048), 0)
    ).astype(F32).astype(BF16)
    mask = jnp.dot(chosen_rows, spread, preferred_element_type=F32)

    position = lax.broadcasted_iota(I32, (8, 2048), 1)
    top_rows = lax.broadcasted_iota(I32, (8, 1), 0) < 4
    scale = 128.0 ** (-0.5)
    nt = (((1,), (1,)), ((), ()))
    for b in range(4):
        q = query_ref[b]
        qf = q.astype(F32)
        fresh = jnp.where(
            top_rows, fresh_ref[b, 0:1, :].astype(F32), fresh_ref[b, 1:2, :].astype(F32)
        )
        own = jnp.sum(qf * fresh, axis=1, keepdims=True) * scale
        live = (mask[b * 8 : (b + 1) * 8] > 0.5) & (position < len_ref[b])
        pltpu.make_async_copy(key_hbm.at[b], key_buf.at[b], kv_sem.at[0, b]).wait()
        s0 = lax.dot_general(q, key_buf[b, 0], nt, preferred_element_type=F32)
        s1 = lax.dot_general(q, key_buf[b, 1], nt, preferred_element_type=F32)
        scores = jnp.where(top_rows, s0, s1) * scale
        masked = jnp.where(live, scores, -1e30)
        top = jnp.maximum(jnp.max(masked, axis=1, keepdims=True), own)
        expo = jnp.where(live, jnp.exp(scores - top), 0.0)
        own_expo = jnp.exp(own - top)
        total = jnp.sum(expo, axis=1, keepdims=True) + own_expo
        weights = (expo / total).astype(BF16)
        own_weight = (own_expo / total).astype(BF16).astype(F32)
        pltpu.make_async_copy(value_hbm.at[b], value_buf.at[b], kv_sem.at[1, b]).wait()
        a0 = jnp.dot(weights, value_buf[b, 0], preferred_element_type=F32)
        a1 = jnp.dot(weights, value_buf[b, 1], preferred_element_type=F32)
        new = jnp.where(
            top_rows, vnew_ref[b, 0:1, :].astype(F32), vnew_ref[b, 1:2, :].astype(F32)
        )
        attn_buf[b * 8 : (b + 1) * 8, :] = (
            jnp.where(top_rows, a0, a1) + own_weight * new
        ).astype(BF16)

    pltpu.make_async_copy(wout_hbm, wout_buf, w_sem.at[0]).start()
    pltpu.make_async_copy(win_hbm.at[0], win_buf, w_sem.at[1]).start()
    pltpu.make_async_copy(wdown_hbm.at[0], wdown_buf, w_sem.at[2]).start()
    here = quarter == h
    pl.semaphore_wait(barrier, 73 - here.astype(I32))
    for j in range(8):
        own_place = here & (h * 8 + j == d)

        @pl.when(own_place)
        def _():
            pltpu.make_async_copy(msg_buf.at[j], recv_m.at[block], recv_sem.at[1]).start()

        @pl.when(jnp.logical_not(own_place))
        def _():
            pltpu.make_async_remote_copy(
                msg_buf.at[j],
                recv_m.at[block],
                send_sem.at[1],
                recv_sem.at[1],
                (h * 8 + j, quarter),
                MESH,
            ).start()

    for i in FAR:
        pltpu.make_async_remote_copy(
            attn_buf, recv_a.at[d], send_sem.at[0], recv_sem.at[0], (d ^ i, h), MESH
        ).start()
    pltpu.make_async_copy(attn_buf, recv_a.at[d], recv_sem.at[0]).start()

    own_gains = recv_g.at[pl.ds(pl.multiple_of(h * 8, 8), 8)]
    for i in range(1, 4):
        pltpu.make_async_remote_copy(
            gain_ref, own_gains, send_sem.at[2], recv_sem.at[2], (d, h ^ i), MESH
        ).start()
    pltpu.make_async_copy(gain_ref, own_gains, recv_sem.at[2]).start()

    whole_wait(recv_m, recv_sem.at[1])
    messages = recv_m[...].astype(F32).reshape(64, 128).astype(BF16)
    pick_row = lax.broadcasted_iota(I32, (40, 64), 0)
    pick_col = lax.broadcasted_iota(I32, (40, 64), 1)
    pick = (
        ((pick_row < 32) & (pick_col == (pick_row >> 2) * 8 + (pick_row & 3)))
        | ((pick_row == 32) & ((pick_col & 7) == 4))
        | ((pick_row == 33) & ((pick_col & 7) == 5))
    )
    picked = jnp.dot(pick.astype(F32).astype(BF16), messages, preferred_element_type=F32)
    residual = picked[:32]
    slot_row = lax.broadcasted_iota(I32, (128, 128), 0).astype(F32)
    select = ((slot_row == picked[32:33]) | (slot_row == picked[33:34])).astype(F32)
    select = select[:, :32].astype(BF16)
    pltpu.make_async_copy(wout_hbm, wout_buf, w_sem.at[0]).wait()

    whole_wait(recv_a, recv_sem.at[0])
    rows_f[...] = recv_a[...].astype(F32).reshape(1024, 128)
    columns = jnp.zeros((128, 128), F32)
    for n in range(4):
        pair = jnp.concatenate(
            [rows_f[pl.ds(n * 2 + m, 128, stride=8), :] for m in range(2)], axis=1
        ).astype(BF16)
        columns = columns + jnp.dot(
            pair, wout_buf[n * 256 : (n + 1) * 256, :], preferred_element_type=F32
        )
    part_buf[...] = columns.astype(BF16).reshape(4, 32, 128)

    for i in range(1, 4):
        to = h ^ i
        pltpu.make_async_remote_copy(
            part_buf.at[to], recv_r.at[h], send_sem.at[3], recv_sem.at[3], (d, to), MESH
        ).start()
    pltpu.make_async_copy(part_buf.at[h], recv_r.at[h], recv_sem.at[3]).start()
    whole_wait(recv_r, recv_sem.at[3])
    stream = residual
    for i in range(4):
        stream = stream + recv_r[i].astype(F32)
    stream_buf[...] = stream.reshape(4, 8, 128)
    sel_buf[...] = (
        jnp.dot(select, stream.astype(BF16), preferred_element_type=F32)
        .astype(BF16)
        .reshape(8, 16, 128)
    )

    slot = block
    for i in FAR + [0]:
        to = d ^ i
        for side in range(2):
            place = recv_b.at[c, (i & 24) + slot, y]

            def remote():
                pltpu.make_async_remote_copy(
                    sel_buf.at[to >> 2],
                    place,
                    send_sem.at[4],
                    group_sem.at[i >> 3],
                    (to, side * 2 + c),
                    MESH,
                ).start()

            if i:
                remote()
            else:
                pl.when(y != side)(remote)
    pltpu.make_async_copy(sel_buf.at[d >> 2], recv_b.at[c, slot, y], group_sem.at[0]).start()

    for b in range(8):
        own_place = here & (h * 8 + b == d)

        @pl.when(own_place)
        def _():
            pltpu.make_async_copy(
                stream_buf.at[b // 2], recv_s.at[block], recv_sem.at[5]
            ).start()

        @pl.when(jnp.logical_not(own_place))
        def _():
            pltpu.make_async_remote_copy(
                stream_buf.at[b // 2],
                recv_s.at[block],
                send_sem.at[5],
                recv_sem.at[5],
                (h * 8 + b, quarter),
                MESH,
            ).start()

    pltpu.make_async_copy(win_hbm.at[0], win_buf, w_sem.at[1]).wait()
    pltpu.make_async_copy(wdown_hbm.at[0], wdown_buf, w_sem.at[2]).wait()
    whole_wait(recv_g, recv_sem.at[2])

    def hand_on(k):
        return pltpu.make_async_remote_copy(
            recv_b.at[c, pl.ds(k * 8, 8)],
            recv_b.at[c, pl.ds(k * 8, 8)],
            pass_send.at[k],
            pass_recv.at[k],
            sibling,
            MESH,
        )

    def arrived(k):
        whole_wait(recv_b.at[c, pl.ds(k * 8, 8)], group_sem.at[k])
        hand_on(k).start()

    squares = jnp.zeros((64, 128), F32)
    gate = jnp.zeros((64, 448), F32)
    up = jnp.zeros((64, 448), F32)
    arrived(ORDER[0])
    for n in range(4):
        k = ORDER[n]
        if n < 3:
            arrived(ORDER[n + 1])
        whole_wait(recv_b.at[1 - c, pl.ds(k * 8, 8)], pass_recv.at[k])
        first = quarter ^ k
        gains = recv_g[pl.ds(pl.multiple_of(first * 8, 8), 8), :]
        for m in range(8):
            x = recv_b[:, k * 8 + m].reshape(64, 128).astype(F32)
            squares = squares + x * x
            x_buf[:, m * 128 : (m + 1) * 128] = (x * gains[m : m + 1]).astype(BF16)
        columns = pl.ds(pl.multiple_of(first * 1024, 1024), 1024)
        x = x_buf[...]
        gate = gate + lax.dot_general(x, win_buf[0, :, columns], nt, preferred_element_type=F32)
        up = up + lax.dot_general(x, win_buf[1, :, columns], nt, preferred_element_type=F32)
    inverse = lax.rsqrt(jnp.sum(squares, axis=1, keepdims=True) * (1.0 / 4096.0) + EPSILON)
    gate = gate * inverse
    hidden = (gate * jax.nn.sigmoid(gate) * (up * inverse)).astype(BF16)

    def slab(side, core):
        base = (side * 2 + core) * 1024
        for n in range(4):
            columns = pl.ds(pl.multiple_of(base + n * 256, 256), 256)
            part = jnp.dot(hidden, wdown_buf[:, columns], preferred_element_type=F32)
            for m in range(2):
                slab_f[pl.ds(n * 2 + m, 64, stride=8), :] = part[:, m * 128 : (m + 1) * 128]
        return slab_f[...]

    def to_sibling(side):
        return pltpu.make_async_remote_copy(
            sib_buf.at[side],
            recv_d.at[side],
            sib_send.at[side],
            sib_recv.at[side],
            sibling,
            MESH,
        )

    for side in range(2):
        sib_buf[side] = slab(side, 1 - c).astype(BF16)
        to_sibling(side).start()
    for side in range(2):
        total = slab(side, c)
        to_sibling(side).wait_recv()
        total = total + recv_d[side].astype(F32)
        slab_b[side] = total.astype(BF16).reshape(32, 16, 128)
        for i in FAR + [0]:
            to = d ^ i
            rows = ((to >> 3) & 1) * 16 + (to >> 4) * 8 + (to & 7)

            def remote():
                pltpu.make_async_remote_copy(
                    slab_b.at[side, rows],
                    recv_c.at[d * 2 + y],
                    send_sem.at[6],
                    recv_sem.at[6],
                    (to, side * 2 + c),
                    MESH,
                ).start()

            if i:
                remote()
            else:
                pl.when(y != side)(remote)
    rows = ((d >> 3) & 1) * 16 + (d >> 4) * 8 + (d & 7)
    pltpu.make_async_copy(slab_b.at[y, rows], recv_c.at[d * 2 + y], recv_sem.at[6]).start()

    slot16 = lax.broadcasted_iota(I32, (16, 128), 0)
    factors = []
    for t in range(4):
        factor = jnp.zeros((16, 128), F32)
        for j in range(2):
            a = t * 2 + j
            factor = factor + jnp.where(slot16 == ids[a] * 2 + slots[a], gates_ref[j, t], 0.0)
        factors.append(factor)
    odd = (d & 1) == 1

    whole_wait(recv_s, recv_sem.at[5])
    whole_wait(recv_c, recv_sem.at[6])
    for e in range(8):
        total = recv_c[e * 8].astype(F32)
        for i in range(1, 8):
            total = total + recv_c[e * 8 + i].astype(F32)
        mix_f[e * 16 : (e + 1) * 16, :] = total
    for j in range(8):
        slot_rows = mix_f[pl.ds(j, 16, stride=8), :]
        mixed = jnp.concatenate(
            [jnp.sum(slot_rows * f, axis=0, keepdims=True) for f in factors], axis=0
        )
        own_stream = recv_s[j]
        own_stream = jnp.where(odd, own_stream[4:], own_stream[:4])
        out_ref[:, j * 128 : (j + 1) * 128] = (own_stream + mixed).astype(BF16)

    result = pltpu.make_async_copy(out_ref, out_hbm, w_sem.at[0])
    result.start()
    whole_wait(recv_a.at[pl.ds(0, 31)], send_sem.at[0])

    @pl.when(here)
    def _():
        whole_wait(recv_m.at[pl.ds(0, 7)], send_sem.at[1])
        whole_wait(recv_s.at[pl.ds(0, 7)], send_sem.at[5])

    @pl.when(jnp.logical_not(here))
    def _():
        whole_wait(recv_m, send_sem.at[1])
        whole_wait(recv_s, send_sem.at[5])

    whole_wait(recv_g.at[pl.ds(0, 24)], send_sem.at[2])
    whole_wait(recv_r.at[pl.ds(0, 3)], send_sem.at[3])
    whole_wait(recv_c.at[pl.ds(0, 63)], send_sem.at[4])
    whole_wait(recv_c.at[pl.ds(0, 63)], send_sem.at[6])
    for k in range(4):
        hand_on(k).wait_send()
    for side in range(2):
        to_sibling(side).wait_send()
    result.wait()


def shards(
    residual,
    query,
    fresh_token_keys,
    value_new,
    key_cache,
    value_cache,
    lengths,
    pages,
    w_out,
    norm_gain,
    expert_ids,
    gate_weights,
    w_in,
    w_down,
):
    hbm = pl.BlockSpec(memory_space=pltpu.HBM)
    gain = norm_gain.reshape(8, 128)
    return pl.pallas_call(
        layer,
        out_shape=jax.ShapeDtypeStruct((4, 1024), BF16),
        in_specs=[hbm] * 14,
        out_specs=pl.BlockSpec(memory_space=OUT_SPACE),
        scratch_shapes=[
            pltpu.SMEM((2, 4), I32),
            pltpu.SMEM((2, 4), F32),
            pltpu.SMEM((4,), I32),
            pltpu.VMEM(residual.shape, BF16),
            pltpu.VMEM(query.shape, BF16),
            pltpu.VMEM(fresh_token_keys.shape, BF16),
            pltpu.VMEM(value_new.shape, BF16),
            pltpu.VMEM(pages.shape, I32),
            pltpu.VMEM(gain.shape, F32),
            pltpu.VMEM((4, 1024), BF16),
            pltpu.VMEM((4, 2, 2048, 128), BF16),
            pltpu.VMEM((4, 2, 2048, 128), BF16),
            pltpu.VMEM((1024, 128), BF16),
            pltpu.VMEM((2, 448, 4096), BF16),
            pltpu.VMEM((448, 4096), BF16),
            pltpu.VMEM((32, 128), BF16),
            pltpu.VMEM((32, 32, 128), BF16),
            pltpu.VMEM((1024, 128), F32),
            pltpu.VMEM((8, 8, 128), BF16),
            pltpu.VMEM((8, 8, 128), BF16),
            pltpu.VMEM((32, 128), F32),
            pltpu.VMEM((4, 32, 128), BF16),
            pltpu.VMEM((4, 32, 128), BF16),
            pltpu.VMEM((4, 8, 128), F32),
            pltpu.VMEM((8, 16, 128), BF16),
            pltpu.VMEM((2, 32, 2, 16, 128), BF16),
            pltpu.VMEM((8, 8, 128), F32),
            pltpu.VMEM((64, 1024), BF16),
            pltpu.VMEM((512, 128), F32),
            pltpu.VMEM((2, 512, 128), BF16),
            pltpu.VMEM((2, 512, 128), BF16),
            pltpu.VMEM((2, 32, 16, 128), BF16),
            pltpu.VMEM((64, 16, 128), BF16),
            pltpu.VMEM((128, 128), F32),
            pltpu.SemaphoreType.DMA((9,)),
            pltpu.SemaphoreType.DMA((2, 4)),
            pltpu.SemaphoreType.DMA((3,)),
            pltpu.SemaphoreType.DMA((7,)),
            pltpu.SemaphoreType.DMA((7,)),
            pltpu.SemaphoreType.DMA((4,)),
            pltpu.SemaphoreType.DMA((4,)),
            pltpu.SemaphoreType.DMA((4,)),
            pltpu.SemaphoreType.DMA((2,)),
            pltpu.SemaphoreType.DMA((2,)),
        ],
        compiler_params=pltpu.CompilerParams(
            collective_id=0, has_side_effects=True, vmem_limit_bytes=67043328
        ),
        name="layer",
    )(
        expert_ids.T,
        gate_weights.T,
        lengths,
        residual,
        query,
        fresh_token_keys,
        value_new,
        pages,
        gain,
        key_cache,
        value_cache,
        w_out,
        jnp.swapaxes(w_in, 2, 3),
        w_down,
    )


def solution(mesh):
    in_specs = (
        P("dp", "head"),
        P("dp", "head", None),
        P("dp", "head", None),
        P("dp", "head", None),
        P("dp", "head", None, None),
        P("dp", "head", None, None),
        P("dp"),
        P("dp", "head", None),
        P("head", "dp"),
        P("head"),
        P("dp", None),
        P("dp", None),
        P("dp", None, None, "head"),
        P("dp", "head", None),
    )
    out_specs = P("dp", "head")
    return jax.shard_map(shards, mesh=mesh, in_specs=in_specs, out_specs=out_specs, check_vma=False)
```

```python
import functools

import jax
import jax.numpy as jnp
from jax import lax
from jax.experimental import pallas as pl
from jax.experimental.pallas import tpu as pltpu
from jax.sharding import PartitionSpec as P

EXPERTS = 8
PAGE = 16
EPSILON = 1e-05
F32 = jnp.float32
BF16 = jnp.bfloat16
I32 = jnp.int32
MESH = pl.DeviceIdType.MESH
FAR = sorted(range(1, 32), key=lambda i: -(2 * (i >> 4) + (0, 1, 2, 1)[i >> 2 & 3] + (0, 1, 2, 1)[i & 3]))
ORDER = (0, 1, 2, 3)
OUT_SPACE = pl.ANY


def whole_wait(ref, sem):
    pltpu.make_async_copy(ref, ref, sem).wait()


def layer(
    ids_hbm,
    gates_hbm,
    len_hbm,
    residual_hbm,
    query_hbm,
    fresh_hbm,
    vnew_hbm,
    pages_hbm,
    gain_hbm,
    key_hbm,
    value_hbm,
    wout_hbm,
    win_hbm,
    wdown_hbm,
    out_hbm,
    ids_ref,
    gates_ref,
    len_ref,
    page_list,
    residual_ref,
    query_ref,
    fresh_ref,
    vnew_ref,
    pages_ref,
    gain_ref,
    out_ref,
    key0,
    key1,
    key2,
    key3,
    value0,
    value1,
    value2,
    value3,
    wout_buf,
    win_buf,
    wdown_buf,
    attn_buf,
    recv_a,
    rows_f,
    msg_buf,
    recv_m,
    recv_g,
    part_f,
    part_buf,
    recv_r,
    stream_buf,
    sel_buf,
    recv_b,
    recv_s,
    x_buf,
    slab_f,
    own_f,
    sib_buf,
    recv_d,
    slab_b,
    recv_c,
    mix_f,
    in_sem,
    kv_sem,
    w_sem,
    send_sem,
    recv_sem,
    half_sem,
    group_sem,
    pass_send,
    pass_recv,
    sib_send,
    sib_recv,
):
    d = lax.axis_index("dp")
    h = lax.axis_index("head")
    y = h >> 1
    c = h & 1
    sibling = (d, h ^ 1)
    quarter = d >> 3
    block = d & 7

    barrier = pltpu.get_barrier_semaphore()

    def greet(to):
        pl.semaphore_signal(barrier, inc=1, device_id=to, device_id_type=MESH)

    small = [
        (ids_hbm, ids_ref),
        (gates_hbm, gates_ref),
        (len_hbm, len_ref),
        (pages_hbm, page_list),
        (pages_hbm, pages_ref),
        (query_hbm, query_ref),
        (fresh_hbm, fresh_ref),
        (residual_hbm, residual_ref),
        (vnew_hbm, vnew_ref),
        (gain_hbm, gain_ref),
    ]
    for n, (source, target) in enumerate(small):
        pltpu.make_async_copy(source, target, in_sem.at[n]).start()

    keys = [key0, key1, key2, key3]
    values = [value0, value1, value2, value3]

    def load_keys(b):
        return pltpu.make_async_copy(key_hbm.at[b], keys[b], kv_sem.at[0, b])

    def load_values(b):
        return pltpu.make_async_copy(value_hbm.at[b], values[b], kv_sem.at[1, b])

    load_keys(0).start()

    for i in FAR:
        for side in range(2):
            greet((d ^ i, side * 2 + c))
    for i in range(1, 4):
        greet((d, h ^ i))
    for j in range(8):

        @pl.when(jnp.logical_not((h * 8 + j == d) & (quarter == h)))
        def _():
            greet((h * 8 + j, quarter))

    load_keys(1).start()
    load_values(0).start()
    load_values(1).start()
    load_keys(2).start()
    load_keys(3).start()
    load_values(2).start()
    load_values(3).start()
    for n, (source, target) in enumerate(small):
        pltpu.make_async_copy(source, target, in_sem.at[n]).wait()

    ids = [ids_ref[j, t] for t in range(4) for j in range(2)]
    slots = []
    for a in range(8):
        earlier = jnp.int32(0)
        for n in range(a):
            earlier = earlier + (ids[n] == ids[a]).astype(I32)
        slots.append(earlier)
    lane = lax.broadcasted_iota(I32, (8, 128), 1)
    row8 = lax.broadcasted_iota(I32, (8, 128), 0)
    target = jnp.zeros((8, 128), I32)
    for t in range(4):
        for j in range(2):
            a = t * 2 + j
            value = ids[a] * 16 + block * 2 + slots[a]
            target = jnp.where((row8 == 4 + j) & (lane == block * 4 + t), value, target)
    target = target.astype(F32)
    for j in range(8):
        res = residual_ref[:, j * 128 : (j + 1) * 128].astype(F32)
        both = jnp.concatenate([res, jnp.zeros((4, 128), F32)], axis=0)
        msg_buf[j] = (both + target).astype(BF16)

    top_rows = lax.broadcasted_iota(I32, (8, 1), 0) < 4
    numbers = jnp.concatenate(
        [jnp.where(top_rows, pages_ref[b, 0:1, :], pages_ref[b, 1:2, :]) for b in range(4)],
        axis=0,
    )
    spread = (
        (lax.broadcasted_iota(I32, (64, 1024), 1) >> 4)
        == lax.broadcasted_iota(I32, (64, 1024), 0)
    ).astype(F32)
    start = jnp.dot(
        numbers.astype(F32).astype(BF16), spread.astype(BF16), preferred_element_type=F32
    )
    position = start.astype(I32) * PAGE + (lax.broadcasted_iota(I32, (32, 1024), 1) & 15)

    scale = 128.0 ** (-0.5)
    nt = (((1,), (1,)), ((), ()))

    def selected(buf, b, k):
        return jnp.concatenate([buf[k, page_list[b, k, n]] for n in range(64)], axis=0)

    def both(ref, b):
        return jnp.where(top_rows, ref[b, 0:1, :].astype(F32), ref[b, 1:2, :].astype(F32))

    def attend(pair):
        rows = jnp.concatenate([query_ref[b] for b in pair], axis=0).astype(F32)
        fresh = jnp.concatenate([both(fresh_ref, b) for b in pair], axis=0)
        own = jnp.sum(rows * fresh, axis=1, keepdims=True) * scale
        live = jnp.concatenate(
            [position[b * 8 : (b + 1) * 8] < len_ref[b] for b in pair], axis=0
        )
        for b in pair:
            load_keys(b).wait()
        scores = []
        for b in pair:
            q = query_ref[b]
            s0 = lax.dot_general(q, selected(keys[b], b, 0), nt, preferred_element_type=F32)
            s1 = lax.dot_general(q, selected(keys[b], b, 1), nt, preferred_element_type=F32)
            scores.append(jnp.where(top_rows, s0, s1))
        scores = jnp.concatenate(scores, axis=0) * scale
        masked = jnp.where(live, scores, -1e30)
        top = jnp.maximum(jnp.max(masked, axis=1, keepdims=True), own)
        expo = jnp.where(live, jnp.exp(scores - top), 0.0)
        own_expo = jnp.exp(own - top)
        total = jnp.sum(expo, axis=1, keepdims=True) + own_expo
        weights = expo / total
        own_weight = (own_expo / total).astype(BF16).astype(F32)
        for b in pair:
            load_values(b).wait()
        for n, b in enumerate(pair):
            w = weights[n * 8 : (n + 1) * 8].astype(BF16)
            a0 = jnp.dot(w, selected(values[b], b, 0), preferred_element_type=F32)
            a1 = jnp.dot(w, selected(values[b], b, 1), preferred_element_type=F32)
            new = own_weight[n * 8 : (n + 1) * 8] * both(vnew_ref, b)
            attn_buf[b // 2, n * 8 : (n + 1) * 8, :] = (
                jnp.where(top_rows, a0, a1) + new
            ).astype(BF16)

    def send_rows(half):
        for i in FAR:
            pltpu.make_async_remote_copy(
                attn_buf.at[half],
                recv_a.at[half, d],
                send_sem.at[0],
                half_sem.at[half],
                (d ^ i, h),
                MESH,
            ).start()
        pltpu.make_async_copy(attn_buf.at[half], recv_a.at[half, d], half_sem.at[half]).start()

    attend((0, 1))
    attend((2, 3))
    here = quarter == h
    pl.semaphore_wait(barrier, 73 - here.astype(I32))
    for j in range(8):
        own_place = here & (h * 8 + j == d)

        @pl.when(own_place)
        def _():
            pltpu.make_async_copy(msg_buf.at[j], recv_m.at[block], recv_sem.at[1]).start()

        @pl.when(jnp.logical_not(own_place))
        def _():
            pltpu.make_async_remote_copy(
                msg_buf.at[j],
                recv_m.at[block],
                send_sem.at[1],
                recv_sem.at[1],
                (h * 8 + j, quarter),
                MESH,
            ).start()

    send_rows(0)
    send_rows(1)
    pltpu.make_async_copy(wout_hbm, wout_buf, w_sem.at[0]).start()
    pltpu.make_async_copy(win_hbm.at[0], win_buf, w_sem.at[1]).start()
    pltpu.make_async_copy(wdown_hbm.at[0], wdown_buf, w_sem.at[2]).start()

    own_gains = recv_g.at[pl.ds(pl.multiple_of(h * 8, 8), 8)]
    for i in range(1, 4):
        pltpu.make_async_remote_copy(
            gain_ref, own_gains, send_sem.at[2], recv_sem.at[2], (d, h ^ i), MESH
        ).start()
    pltpu.make_async_copy(gain_ref, own_gains, recv_sem.at[2]).start()

    whole_wait(recv_m, recv_sem.at[1])
    messages = recv_m[...].astype(F32).reshape(64, 128).astype(BF16)
    pick_row = lax.broadcasted_iota(I32, (40, 64), 0)
    pick_col = lax.broadcasted_iota(I32, (40, 64), 1)
    pick = (
        ((pick_row < 32) & (pick_col == (pick_row >> 2) * 8 + (pick_row & 3)))
        | ((pick_row == 32) & ((pick_col & 7) == 4))
        | ((pick_row == 33) & ((pick_col & 7) == 5))
    )
    picked = jnp.dot(pick.astype(F32).astype(BF16), messages, preferred_element_type=F32)
    residual = picked[:32]
    slot_row = lax.broadcasted_iota(I32, (128, 128), 0).astype(F32)
    select = ((slot_row == picked[32:33]) | (slot_row == picked[33:34])).astype(F32)
    select = select[:, :32].astype(BF16)
    pltpu.make_async_copy(wout_hbm, wout_buf, w_sem.at[0]).wait()

    def project(half):
        whole_wait(recv_a.at[half], half_sem.at[half])
        rows_f[...] = recv_a[half].astype(F32).reshape(512, 128)
        columns = jnp.zeros((64, 128), F32)
        for n in range(4):
            pair = [
                jnp.concatenate(
                    [rows_f[pl.ds(t * 8 + n * 2 + m, 32, stride=16), :] for t in range(2)], axis=0
                )
                for m in range(2)
            ]
            columns = columns + jnp.dot(
                jnp.concatenate(pair, axis=1).astype(BF16),
                wout_buf[n * 256 : (n + 1) * 256, :],
                preferred_element_type=F32,
            )
        for t in range(2):
            part_f[pl.ds(half * 2 + t, 32, stride=4), :] = columns[t * 32 : (t + 1) * 32]

    project(0)
    project(1)
    part_buf[...] = part_f[...].astype(BF16).reshape(4, 32, 128)

    for i in range(1, 4):
        to = h ^ i
        pltpu.make_async_remote_copy(
            part_buf.at[to], recv_r.at[h], send_sem.at[3], recv_sem.at[3], (d, to), MESH
        ).start()
    pltpu.make_async_copy(part_buf.at[h], recv_r.at[h], recv_sem.at[3]).start()
    whole_wait(recv_r, recv_sem.at[3])
    stream = residual
    for i in range(4):
        stream = stream + recv_r[i].astype(F32)
    stream_buf[...] = stream.reshape(4, 8, 128)
    sel_buf[...] = (
        jnp.dot(select, stream.astype(BF16), preferred_element_type=F32)
        .astype(BF16)
        .reshape(8, 16, 128)
    )

    slot = block
    for i in range(32):
        to = d ^ i
        for side in range(2):
            place = recv_b.at[c, (i & 24) + slot, y]

            def remote():
                pltpu.make_async_remote_copy(
                    sel_buf.at[to >> 2],
                    place,
                    send_sem.at[4],
                    group_sem.at[i >> 3],
                    (to, side * 2 + c),
                    MESH,
                ).start()

            if i:
                remote()
            else:
                pl.when(y != side)(remote)
    pltpu.make_async_copy(sel_buf.at[d >> 2], recv_b.at[c, slot, y], group_sem.at[0]).start()

    for b in range(8):
        own_place = here & (h * 8 + b == d)

        @pl.when(own_place)
        def _():
            pltpu.make_async_copy(
                stream_buf.at[b // 2], recv_s.at[block], recv_sem.at[5]
            ).start()

        @pl.when(jnp.logical_not(own_place))
        def _():
            pltpu.make_async_remote_copy(
                stream_buf.at[b // 2],
                recv_s.at[block],
                send_sem.at[5],
                recv_sem.at[5],
                (h * 8 + b, quarter),
                MESH,
            ).start()

    pltpu.make_async_copy(win_hbm.at[0], win_buf, w_sem.at[1]).wait()
    pltpu.make_async_copy(wdown_hbm.at[0], wdown_buf, w_sem.at[2]).wait()
    whole_wait(recv_g, recv_sem.at[2])

    def hand_on(k):
        return pltpu.make_async_remote_copy(
            recv_b.at[c, pl.ds(k * 8, 8)],
            recv_b.at[c, pl.ds(k * 8, 8)],
            pass_send.at[k],
            pass_recv.at[k],
            sibling,
            MESH,
        )

    def arrived(k):
        whole_wait(recv_b.at[c, pl.ds(k * 8, 8)], group_sem.at[k])
        hand_on(k).start()

    squares = jnp.zeros((64, 128), F32)
    gate = jnp.zeros((64, 448), F32)
    up = jnp.zeros((64, 448), F32)
    arrived(ORDER[0])
    for n in range(4):
        k = ORDER[n]
        if n < 3:
            arrived(ORDER[n + 1])
        whole_wait(recv_b.at[1 - c, pl.ds(k * 8, 8)], pass_recv.at[k])
        first = quarter ^ k
        gains = recv_g[pl.ds(pl.multiple_of(first * 8, 8), 8), :]
        for m in range(8):
            x = recv_b[:, k * 8 + m].reshape(64, 128).astype(F32)
            squares = squares + x * x
            x_buf[:, m * 128 : (m + 1) * 128] = (x * gains[m : m + 1]).astype(BF16)
        columns = pl.ds(pl.multiple_of(first * 1024, 1024), 1024)
        x = x_buf[...]
        gate = gate + lax.dot_general(x, win_buf[0, :, columns], nt, preferred_element_type=F32)
        up = up + lax.dot_general(x, win_buf[1, :, columns], nt, preferred_element_type=F32)
    inverse = lax.rsqrt(jnp.sum(squares, axis=1, keepdims=True) * (1.0 / 4096.0) + EPSILON)
    gate = gate * inverse
    hidden = (gate * jax.nn.sigmoid(gate) * (up * inverse)).astype(BF16)

    def slab(side, core):
        base = (side * 2 + core) * 1024
        for n in range(4):
            columns = pl.ds(pl.multiple_of(base + n * 256, 256), 256)
            part = jnp.dot(hidden, wdown_buf[:, columns], preferred_element_type=F32)
            for m in range(2):
                slab_f[pl.ds(n * 2 + m, 64, stride=8), :] = part[:, m * 128 : (m + 1) * 128]
        return slab_f[...]

    def to_sibling(side):
        return pltpu.make_async_remote_copy(
            sib_buf.at[side],
            recv_d.at[side],
            sib_send.at[side],
            sib_recv.at[side],
            sibling,
            MESH,
        )

    for side in range(2):
        sib_buf[side] = slab(side, 1 - c).astype(BF16)
        to_sibling(side).start()
    for side in range(2):
        own_f[side] = slab(side, c)
    for side in range(2):
        to_sibling(side).wait_recv()
        total = own_f[side] + recv_d[side].astype(F32)
        slab_b[side] = total.astype(BF16).reshape(32, 16, 128)
        for i in FAR + [0]:
            to = d ^ i
            rows = ((to >> 3) & 1) * 16 + (to >> 4) * 8 + (to & 7)

            def remote():
                pltpu.make_async_remote_copy(
                    slab_b.at[side, rows],
                    recv_c.at[d * 2 + y],
                    send_sem.at[6],
                    recv_sem.at[6],
                    (to, side * 2 + c),
                    MESH,
                ).start()

            if i:
                remote()
            else:
                pl.when(y != side)(remote)
    rows = ((d >> 3) & 1) * 16 + (d >> 4) * 8 + (d & 7)
    pltpu.make_async_copy(slab_b.at[y, rows], recv_c.at[d * 2 + y], recv_sem.at[6]).start()

    slot16 = lax.broadcasted_iota(I32, (16, 128), 0)
    factors = []
    for t in range(4):
        factor = jnp.zeros((16, 128), F32)
        for j in range(2):
            a = t * 2 + j
            factor = factor + jnp.where(slot16 == ids[a] * 2 + slots[a], gates_ref[j, t], 0.0)
        factors.append(factor)
    odd = (d & 1) == 1

    whole_wait(recv_s, recv_sem.at[5])
    whole_wait(recv_c, recv_sem.at[6])
    for e in range(8):
        total = recv_c[e * 8].astype(F32)
        for i in range(1, 8):
            total = total + recv_c[e * 8 + i].astype(F32)
        mix_f[e * 16 : (e + 1) * 16, :] = total
    for j in range(8):
        slot_rows = mix_f[pl.ds(j, 16, stride=8), :]
        mixed = jnp.concatenate(
            [jnp.sum(slot_rows * f, axis=0, keepdims=True) for f in factors], axis=0
        )
        own_stream = recv_s[j]
        own_stream = jnp.where(odd, own_stream[4:], own_stream[:4])
        out_ref[:, j * 128 : (j + 1) * 128] = (own_stream + mixed).astype(BF16)

    result = pltpu.make_async_copy(out_ref, out_hbm, w_sem.at[0])
    result.start()
    for half in range(2):
        whole_wait(recv_a.at[half, pl.ds(0, 31)], send_sem.at[0])

    @pl.when(here)
    def _():
        whole_wait(recv_m.at[pl.ds(0, 7)], send_sem.at[1])
        whole_wait(recv_s.at[pl.ds(0, 7)], send_sem.at[5])

    @pl.when(jnp.logical_not(here))
    def _():
        whole_wait(recv_m, send_sem.at[1])
        whole_wait(recv_s, send_sem.at[5])

    whole_wait(recv_g.at[pl.ds(0, 24)], send_sem.at[2])
    whole_wait(recv_r.at[pl.ds(0, 3)], send_sem.at[3])
    whole_wait(recv_c.at[pl.ds(0, 63)], send_sem.at[4])
    whole_wait(recv_c.at[pl.ds(0, 63)], send_sem.at[6])
    for k in range(4):
        hand_on(k).wait_send()
    for side in range(2):
        to_sibling(side).wait_send()
    result.wait()


def shards(
    residual,
    query,
    fresh_token_keys,
    value_new,
    key_cache,
    value_cache,
    lengths,
    pages,
    w_out,
    norm_gain,
    expert_ids,
    gate_weights,
    w_in,
    w_down,
):
    hbm = pl.BlockSpec(memory_space=pltpu.HBM)
    gain = norm_gain.reshape(8, 128)
    return pl.pallas_call(
        layer,
        out_shape=jax.ShapeDtypeStruct((4, 1024), BF16),
        in_specs=[hbm] * 14,
        out_specs=pl.BlockSpec(memory_space=OUT_SPACE),
        scratch_shapes=[
            pltpu.SMEM((2, 4), I32),
            pltpu.SMEM((2, 4), F32),
            pltpu.SMEM((4,), I32),
            pltpu.SMEM(pages.shape, I32),
            pltpu.VMEM(residual.shape, BF16),
            pltpu.VMEM(query.shape, BF16),
            pltpu.VMEM(fresh_token_keys.shape, BF16),
            pltpu.VMEM(value_new.shape, BF16),
            pltpu.VMEM(pages.shape, I32),
            pltpu.VMEM(gain.shape, F32),
            pltpu.VMEM((4, 1024), BF16),
        ]
        + [pltpu.VMEM((2, 128, PAGE, 128), BF16)] * 8
        + [
            pltpu.VMEM((1024, 128), BF16),
            pltpu.VMEM((2, 448, 4096), BF16),
            pltpu.VMEM((448, 4096), BF16),
            pltpu.VMEM((2, 16, 128), BF16),
            pltpu.VMEM((2, 32, 16, 128), BF16),
            pltpu.VMEM((512, 128), F32),
            pltpu.VMEM((8, 8, 128), BF16),
            pltpu.VMEM((8, 8, 128), BF16),
            pltpu.VMEM((32, 128), F32),
            pltpu.VMEM((128, 128), F32),
            pltpu.VMEM((4, 32, 128), BF16),
            pltpu.VMEM((4, 32, 128), BF16),
            pltpu.VMEM((4, 8, 128), F32),
            pltpu.VMEM((8, 16, 128), BF16),
            pltpu.VMEM((2, 32, 2, 16, 128), BF16),
            pltpu.VMEM((8, 8, 128), F32),
            pltpu.VMEM((64, 1024), BF16),
            pltpu.VMEM((512, 128), F32),
            pltpu.VMEM((2, 512, 128), F32),
            pltpu.VMEM((2, 512, 128), BF16),
            pltpu.VMEM((2, 512, 128), BF16),
            pltpu.VMEM((2, 32, 16, 128), BF16),
            pltpu.VMEM((64, 16, 128), BF16),
            pltpu.VMEM((128, 128), F32),
            pltpu.SemaphoreType.DMA((10,)),
            pltpu.SemaphoreType.DMA((2, 4)),
            pltpu.SemaphoreType.DMA((3,)),
            pltpu.SemaphoreType.DMA((7,)),
            pltpu.SemaphoreType.DMA((7,)),
            pltpu.SemaphoreType.DMA((2,)),
            pltpu.SemaphoreType.DMA((4,)),
            pltpu.SemaphoreType.DMA((4,)),
            pltpu.SemaphoreType.DMA((4,)),
            pltpu.SemaphoreType.DMA((2,)),
            pltpu.SemaphoreType.DMA((2,)),
        ],
        compiler_params=pltpu.CompilerParams(
            collective_id=0, has_side_effects=True, vmem_limit_bytes=67043328
        ),
        name="layer",
    )(
        expert_ids.T,
        gate_weights.T,
        lengths,
        residual,
        query,
        fresh_token_keys,
        value_new,
        pages,
        gain,
        key_cache.reshape(4, 2, 128, PAGE, 128),
        value_cache.reshape(4, 2, 128, PAGE, 128),
        w_out,
        jnp.swapaxes(w_in, 2, 3),
        w_down,
    )


def solution(mesh):
    in_specs = (
        P("dp", "head"),
        P("dp", "head", None),
        P("dp", "head", None),
        P("dp", "head", None),
        P("dp", "head", None, None),
        P("dp", "head", None, None),
        P("dp"),
        P("dp", "head", None),
        P("head", "dp"),
        P("head"),
        P("dp", None),
        P("dp", None),
        P("dp", None, None, "head"),
        P("dp", "head", None),
    )
    out_specs = P("dp", "head")
    return jax.shard_map(shards, mesh=mesh, in_specs=in_specs, out_specs=out_specs, check_vma=False)
```

```python
import functools

import jax
import jax.numpy as jnp
from jax import lax
from jax.experimental import pallas as pl
from jax.experimental.pallas import tpu as pltpu
from jax.sharding import PartitionSpec as P

EXPERTS = 8
PAGE = 16
EPSILON = 1e-05
F32 = jnp.float32
BF16 = jnp.bfloat16
I32 = jnp.int32
MESH = pl.DeviceIdType.MESH
FAR = sorted(range(1, 32), key=lambda i: -(2 * (i >> 4) + (0, 1, 2, 1)[i >> 2 & 3] + (0, 1, 2, 1)[i & 3]))
ORDER = (0, 1, 2, 3)
OUT_SPACE = pl.ANY


def whole_wait(ref, sem):
    pltpu.make_async_copy(ref, ref, sem).wait()


def layer(
    ids_hbm,
    gates_hbm,
    len_hbm,
    residual_hbm,
    query_hbm,
    fresh_hbm,
    vnew_hbm,
    pages_hbm,
    gain_hbm,
    key_hbm,
    value_hbm,
    wout_hbm,
    win_hbm,
    wdown_hbm,
    out_hbm,
    ids_ref,
    gates_ref,
    len_ref,
    page_list,
    residual_ref,
    query_ref,
    fresh_ref,
    vnew_ref,
    pages_ref,
    gain_ref,
    out_ref,
    key0,
    key1,
    key2,
    key3,
    value0,
    value1,
    value2,
    value3,
    wout_buf,
    win_buf,
    turned,
    wdown_buf,
    attn_buf,
    recv_a,
    rows_f,
    msg_buf,
    recv_m,
    recv_g,
    part_buf,
    recv_r,
    stream_buf,
    sel_buf,
    recv_b,
    recv_s,
    x_buf,
    slab_f,
    own_f,
    sib_buf,
    recv_d,
    slab_b,
    recv_c,
    mix_f,
    in_sem,
    kv_sem,
    w_sem,
    send_sem,
    recv_sem,
    group_sem,
    pass_send,
    pass_recv,
    sib_send,
    sib_recv,
):
    d = lax.axis_index("dp")
    h = lax.axis_index("head")
    y = h >> 1
    c = h & 1
    sibling = (d, h ^ 1)
    quarter = d >> 3
    block = d & 7

    barrier = pltpu.get_barrier_semaphore()

    def greet(to):
        pl.semaphore_signal(barrier, inc=1, device_id=to, device_id_type=MESH)

    small = [
        (ids_hbm, ids_ref),
        (gates_hbm, gates_ref),
        (len_hbm, len_ref),
        (pages_hbm, page_list),
        (pages_hbm, pages_ref),
        (query_hbm, query_ref),
        (fresh_hbm, fresh_ref),
        (residual_hbm, residual_ref),
        (vnew_hbm, vnew_ref),
        (gain_hbm, gain_ref),
    ]
    for n, (source, target) in enumerate(small):
        pltpu.make_async_copy(source, target, in_sem.at[n]).start()

    keys = [key0, key1, key2, key3]
    values = [value0, value1, value2, value3]

    def load_keys(b):
        return pltpu.make_async_copy(key_hbm.at[b], keys[b], kv_sem.at[0, b])

    def load_values(b):
        return pltpu.make_async_copy(value_hbm.at[b], values[b], kv_sem.at[1, b])

    load_keys(0).start()
    load_keys(1).start()

    for i in FAR:
        for side in range(2):
            greet((d ^ i, side * 2 + c))
    for i in range(1, 4):
        greet((d, h ^ i))
    for j in range(8):

        @pl.when(jnp.logical_not((h * 8 + j == d) & (quarter == h)))
        def _():
            greet((h * 8 + j, quarter))

    for b in range(2, 4):
        load_keys(b).start()
    for b in range(4):
        load_values(b).start()
    for n, (source, target) in enumerate(small):
        pltpu.make_async_copy(source, target, in_sem.at[n]).wait()

    ids = [ids_ref[j, t] for t in range(4) for j in range(2)]
    slots = []
    for a in range(8):
        earlier = jnp.int32(0)
        for n in range(a):
            earlier = earlier + (ids[n] == ids[a]).astype(I32)
        slots.append(earlier)
    lane = lax.broadcasted_iota(I32, (8, 128), 1)
    row8 = lax.broadcasted_iota(I32, (8, 128), 0)
    target = jnp.zeros((8, 128), I32)
    for t in range(4):
        for j in range(2):
            a = t * 2 + j
            value = ids[a] * 16 + block * 2 + slots[a]
            target = jnp.where((row8 == 4 + j) & (lane == block * 4 + t), value, target)
    target = target.astype(F32)
    for j in range(8):
        res = residual_ref[:, j * 128 : (j + 1) * 128].astype(F32)
        both = jnp.concatenate([res, jnp.zeros((4, 128), F32)], axis=0)
        msg_buf[j] = (both + target).astype(BF16)

    top_rows = lax.broadcasted_iota(I32, (8, 1), 0) < 4
    numbers = jnp.concatenate(
        [jnp.where(top_rows, pages_ref[b, 0:1, :], pages_ref[b, 1:2, :]) for b in range(4)],
        axis=0,
    )
    spread = (
        (lax.broadcasted_iota(I32, (64, 1024), 1) >> 4)
        == lax.broadcasted_iota(I32, (64, 1024), 0)
    ).astype(F32)
    start = jnp.dot(
        numbers.astype(F32).astype(BF16), spread.astype(BF16), preferred_element_type=F32
    )
    position = start.astype(I32) * PAGE + (lax.broadcasted_iota(I32, (32, 1024), 1) & 15)

    scale = 128.0 ** (-0.5)
    nt = (((1,), (1,)), ((), ()))

    def selected(buf, b, k):
        return jnp.concatenate([buf[k, page_list[b, k, n]] for n in range(64)], axis=0)

    def both(ref, b):
        return jnp.where(top_rows, ref[b, 0:1, :].astype(F32), ref[b, 1:2, :].astype(F32))

    def attend(pair):
        rows = jnp.concatenate([query_ref[b] for b in pair], axis=0).astype(F32)
        fresh = jnp.concatenate([both(fresh_ref, b) for b in pair], axis=0)
        own = jnp.sum(rows * fresh, axis=1, keepdims=True) * scale
        live = jnp.concatenate(
            [position[b * 8 : (b + 1) * 8] < len_ref[b] for b in pair], axis=0
        )
        scores = []
        for b in pair:
            load_keys(b).wait()
            q = query_ref[b]
            s0 = lax.dot_general(q, selected(keys[b], b, 0), nt, preferred_element_type=F32)
            s1 = lax.dot_general(q, selected(keys[b], b, 1), nt, preferred_element_type=F32)
            scores.append(jnp.where(top_rows, s0, s1))
        scores = jnp.concatenate(scores, axis=0) * scale
        masked = jnp.where(live, scores, -1e30)
        top = jnp.maximum(jnp.max(masked, axis=1, keepdims=True), own)
        expo = jnp.where(live, jnp.exp(scores - top), 0.0)
        own_expo = jnp.exp(own - top)
        total = jnp.sum(expo, axis=1, keepdims=True) + own_expo
        weights = expo / total
        own_weight = (own_expo / total).astype(BF16).astype(F32)
        for n, b in enumerate(pair):
            load_values(b).wait()
            w = weights[n * 8 : (n + 1) * 8].astype(BF16)
            a0 = jnp.dot(w, selected(values[b], b, 0), preferred_element_type=F32)
            a1 = jnp.dot(w, selected(values[b], b, 1), preferred_element_type=F32)
            new = own_weight[n * 8 : (n + 1) * 8] * both(vnew_ref, b)
            attn_buf[n * 8 : (n + 1) * 8, :] = (
                jnp.where(top_rows, a0, a1) + new
            ).astype(BF16)

    def send_rows():
        for i in FAR:
            pltpu.make_async_remote_copy(
                attn_buf, recv_a.at[d], send_sem.at[0], recv_sem.at[0], (d ^ i, h), MESH
            ).start()
        pltpu.make_async_copy(attn_buf, recv_a.at[d], recv_sem.at[0]).start()

    attend(range(4))
    pltpu.make_async_copy(wout_hbm, wout_buf, w_sem.at[0]).start()
    pltpu.make_async_copy(win_hbm.at[0], win_buf, w_sem.at[1]).start()
    pltpu.make_async_copy(wdown_hbm.at[0], wdown_buf, w_sem.at[2]).start()
    here = quarter == h
    pl.semaphore_wait(barrier, 73 - here.astype(I32))
    for j in range(8):
        own_place = here & (h * 8 + j == d)

        @pl.when(own_place)
        def _():
            pltpu.make_async_copy(msg_buf.at[j], recv_m.at[block], recv_sem.at[1]).start()

        @pl.when(jnp.logical_not(own_place))
        def _():
            pltpu.make_async_remote_copy(
                msg_buf.at[j],
                recv_m.at[block],
                send_sem.at[1],
                recv_sem.at[1],
                (h * 8 + j, quarter),
                MESH,
            ).start()

    send_rows()

    own_gains = recv_g.at[pl.ds(pl.multiple_of(h * 8, 8), 8)]
    for i in range(1, 4):
        pltpu.make_async_remote_copy(
            gain_ref, own_gains, send_sem.at[2], recv_sem.at[2], (d, h ^ i), MESH
        ).start()
    pltpu.make_async_copy(gain_ref, own_gains, recv_sem.at[2]).start()

    pltpu.make_async_copy(win_hbm.at[0], win_buf, w_sem.at[1]).wait()
    identity = (
        lax.broadcasted_iota(I32, (256, 256), 0) == lax.broadcasted_iota(I32, (256, 256), 1)
    ).astype(F32).astype(BF16)
    for m in range(2):
        for n in range(16):
            part = win_buf[m, :, n * 256 : (n + 1) * 256]
            turned[m, n * 256 : (n + 1) * 256, :] = lax.dot_general(
                identity, part, nt, preferred_element_type=F32
            ).astype(BF16)

    whole_wait(recv_m, recv_sem.at[1])
    messages = recv_m[...].astype(F32).reshape(64, 128).astype(BF16)
    pick_row = lax.broadcasted_iota(I32, (40, 64), 0)
    pick_col = lax.broadcasted_iota(I32, (40, 64), 1)
    pick = (
        ((pick_row < 32) & (pick_col == (pick_row >> 2) * 8 + (pick_row & 3)))
        | ((pick_row == 32) & ((pick_col & 7) == 4))
        | ((pick_row == 33) & ((pick_col & 7) == 5))
    )
    picked = jnp.dot(pick.astype(F32).astype(BF16), messages, preferred_element_type=F32)
    residual = picked[:32]
    slot_row = lax.broadcasted_iota(I32, (128, 128), 0).astype(F32)
    select = ((slot_row == picked[32:33]) | (slot_row == picked[33:34])).astype(F32)
    select = select[:, :32].astype(BF16)
    pltpu.make_async_copy(wout_hbm, wout_buf, w_sem.at[0]).wait()

    whole_wait(recv_a, recv_sem.at[0])
    rows_f[...] = recv_a[...].astype(F32).reshape(1024, 128)
    columns = jnp.zeros((128, 128), F32)
    for n in range(4):
        pair = jnp.concatenate(
            [rows_f[pl.ds(n * 2 + m, 128, stride=8), :] for m in range(2)], axis=1
        ).astype(BF16)
        columns = columns + jnp.dot(
            pair, wout_buf[n * 256 : (n + 1) * 256, :], preferred_element_type=F32
        )
    part_buf[...] = columns.astype(BF16).reshape(4, 32, 128)

    for i in range(1, 4):
        to = h ^ i
        pltpu.make_async_remote_copy(
            part_buf.at[to], recv_r.at[h], send_sem.at[3], recv_sem.at[3], (d, to), MESH
        ).start()
    pltpu.make_async_copy(part_buf.at[h], recv_r.at[h], recv_sem.at[3]).start()
    whole_wait(recv_r, recv_sem.at[3])
    stream = residual
    for i in range(4):
        stream = stream + recv_r[i].astype(F32)
    stream_buf[...] = stream.reshape(4, 8, 128)
    sel_buf[...] = (
        jnp.dot(select, stream.astype(BF16), preferred_element_type=F32)
        .astype(BF16)
        .reshape(8, 16, 128)
    )

    slot = block
    for i in range(32):
        to = d ^ i
        for side in range(2):
            place = recv_b.at[c, (i & 24) + slot, y]

            def remote():
                pltpu.make_async_remote_copy(
                    sel_buf.at[to >> 2],
                    place,
                    send_sem.at[4],
                    group_sem.at[i >> 3],
                    (to, side * 2 + c),
                    MESH,
                ).start()

            if i:
                remote()
            else:
                pl.when(y != side)(remote)
    pltpu.make_async_copy(sel_buf.at[d >> 2], recv_b.at[c, slot, y], group_sem.at[0]).start()

    for b in range(8):
        own_place = here & (h * 8 + b == d)

        @pl.when(own_place)
        def _():
            pltpu.make_async_copy(
                stream_buf.at[b // 2], recv_s.at[block], recv_sem.at[5]
            ).start()

        @pl.when(jnp.logical_not(own_place))
        def _():
            pltpu.make_async_remote_copy(
                stream_buf.at[b // 2],
                recv_s.at[block],
                send_sem.at[5],
                recv_sem.at[5],
                (h * 8 + b, quarter),
                MESH,
            ).start()

    pltpu.make_async_copy(wdown_hbm.at[0], wdown_buf, w_sem.at[2]).wait()
    whole_wait(recv_g, recv_sem.at[2])

    def hand_on(k):
        return pltpu.make_async_remote_copy(
            recv_b.at[c, pl.ds(k * 8, 8)],
            recv_b.at[c, pl.ds(k * 8, 8)],
            pass_send.at[k],
            pass_recv.at[k],
            sibling,
            MESH,
        )

    def arrived(k):
        whole_wait(recv_b.at[c, pl.ds(k * 8, 8)], group_sem.at[k])
        hand_on(k).start()

    squares = jnp.zeros((64, 128), F32)
    gate = jnp.zeros((64, 448), F32)
    up = jnp.zeros((64, 448), F32)
    arrived(ORDER[0])
    for n in range(4):
        k = ORDER[n]
        if n < 3:
            arrived(ORDER[n + 1])
        whole_wait(recv_b.at[1 - c, pl.ds(k * 8, 8)], pass_recv.at[k])
        first = quarter ^ k
        gains = recv_g[pl.ds(pl.multiple_of(first * 8, 8), 8), :]
        for m in range(8):
            x = recv_b[:, k * 8 + m].reshape(64, 128).astype(F32)
            squares = squares + x * x
            x_buf[:, m * 128 : (m + 1) * 128] = (x * gains[m : m + 1]).astype(BF16)
        columns = pl.ds(pl.multiple_of(first * 1024, 1024), 1024)
        x = x_buf[...]
        gate = gate + jnp.dot(x, turned[0, columns], preferred_element_type=F32)
        up = up + jnp.dot(x, turned[1, columns], preferred_element_type=F32)
    inverse = lax.rsqrt(jnp.sum(squares, axis=1, keepdims=True) * (1.0 / 4096.0) + EPSILON)
    gate = gate * inverse
    hidden = (gate * jax.nn.sigmoid(gate) * (up * inverse)).astype(BF16)

    def slab(side, core, store):
        base = (side * 2 + core) * 1024
        for n in range(4):
            columns = pl.ds(pl.multiple_of(base + n * 256, 256), 256)
            part = jnp.dot(hidden, wdown_buf[:, columns], preferred_element_type=F32)
            for m in range(2):
                store[pl.ds(n * 2 + m, 64, stride=8), :] = part[:, m * 128 : (m + 1) * 128]
        return store[...]

    def to_sibling(side):
        return pltpu.make_async_remote_copy(
            sib_buf.at[side],
            recv_d.at[side],
            sib_send.at[side],
            sib_recv.at[side],
            sibling,
            MESH,
        )

    for side in range(2):
        sib_buf[side] = slab(side, 1 - c, slab_f.at[side]).astype(BF16)
        to_sibling(side).start()
    for side in range(2):
        slab(side, c, own_f.at[side])
    for side in range(2):
        to_sibling(side).wait_recv()
        total = own_f[side] + recv_d[side].astype(F32)
        slab_b[side] = total.astype(BF16).reshape(32, 16, 128)
        for i in FAR + [0]:
            to = d ^ i
            rows = ((to >> 3) & 1) * 16 + (to >> 4) * 8 + (to & 7)

            def remote():
                pltpu.make_async_remote_copy(
                    slab_b.at[side, rows],
                    recv_c.at[d * 2 + y],
                    send_sem.at[6],
                    recv_sem.at[6],
                    (to, side * 2 + c),
                    MESH,
                ).start()

            if i:
                remote()
            else:
                pl.when(y != side)(remote)
    rows = ((d >> 3) & 1) * 16 + (d >> 4) * 8 + (d & 7)
    pltpu.make_async_copy(slab_b.at[y, rows], recv_c.at[d * 2 + y], recv_sem.at[6]).start()

    slot16 = lax.broadcasted_iota(I32, (16, 128), 0)
    factors = []
    for t in range(4):
        factor = jnp.zeros((16, 128), F32)
        for j in range(2):
            a = t * 2 + j
            factor = factor + jnp.where(slot16 == ids[a] * 2 + slots[a], gates_ref[j, t], 0.0)
        factors.append(factor)
    odd = (d & 1) == 1

    whole_wait(recv_s, recv_sem.at[5])
    whole_wait(recv_c, recv_sem.at[6])
    for e in range(8):
        total = recv_c[e * 8].astype(F32)
        for i in range(1, 8):
            total = total + recv_c[e * 8 + i].astype(F32)
        mix_f[e * 16 : (e + 1) * 16, :] = total
    for j in range(8):
        slot_rows = mix_f[pl.ds(j, 16, stride=8), :]
        mixed = jnp.concatenate(
            [jnp.sum(slot_rows * f, axis=0, keepdims=True) for f in factors], axis=0
        )
        own_stream = recv_s[j]
        own_stream = jnp.where(odd, own_stream[4:], own_stream[:4])
        out_ref[:, j * 128 : (j + 1) * 128] = (own_stream + mixed).astype(BF16)

    result = pltpu.make_async_copy(out_ref, out_hbm, w_sem.at[0])
    result.start()
    whole_wait(recv_a.at[pl.ds(0, 31)], send_sem.at[0])

    @pl.when(here)
    def _():
        whole_wait(recv_m.at[pl.ds(0, 7)], send_sem.at[1])
        whole_wait(recv_s.at[pl.ds(0, 7)], send_sem.at[5])

    @pl.when(jnp.logical_not(here))
    def _():
        whole_wait(recv_m, send_sem.at[1])
        whole_wait(recv_s, send_sem.at[5])

    whole_wait(recv_g.at[pl.ds(0, 24)], send_sem.at[2])
    whole_wait(recv_r.at[pl.ds(0, 3)], send_sem.at[3])
    whole_wait(recv_c.at[pl.ds(0, 63)], send_sem.at[4])
    whole_wait(recv_c.at[pl.ds(0, 63)], send_sem.at[6])
    for k in range(4):
        hand_on(k).wait_send()
    for side in range(2):
        to_sibling(side).wait_send()
    result.wait()


def shards(
    residual,
    query,
    fresh_token_keys,
    value_new,
    key_cache,
    value_cache,
    lengths,
    pages,
    w_out,
    norm_gain,
    expert_ids,
    gate_weights,
    w_in,
    w_down,
):
    hbm = pl.BlockSpec(memory_space=pltpu.HBM)
    gain = norm_gain.reshape(8, 128)
    return pl.pallas_call(
        layer,
        out_shape=jax.ShapeDtypeStruct((4, 1024), BF16),
        in_specs=[hbm] * 14,
        out_specs=pl.BlockSpec(memory_space=OUT_SPACE),
        scratch_shapes=[
            pltpu.SMEM((2, 4), I32),
            pltpu.SMEM((2, 4), F32),
            pltpu.SMEM((4,), I32),
            pltpu.SMEM(pages.shape, I32),
            pltpu.VMEM(residual.shape, BF16),
            pltpu.VMEM(query.shape, BF16),
            pltpu.VMEM(fresh_token_keys.shape, BF16),
            pltpu.VMEM(value_new.shape, BF16),
            pltpu.VMEM(pages.shape, I32),
            pltpu.VMEM(gain.shape, F32),
            pltpu.VMEM((4, 1024), BF16),
        ]
        + [pltpu.VMEM((2, 128, PAGE, 128), BF16)] * 8
        + [
            pltpu.VMEM((1024, 128), BF16),
            pltpu.VMEM((2, 448, 4096), BF16),
            pltpu.VMEM((2, 4096, 448), BF16),
            pltpu.VMEM((448, 4096), BF16),
            pltpu.VMEM((32, 128), BF16),
            pltpu.VMEM((32, 32, 128), BF16),
            pltpu.VMEM((1024, 128), F32),
            pltpu.VMEM((8, 8, 128), BF16),
            pltpu.VMEM((8, 8, 128), BF16),
            pltpu.VMEM((32, 128), F32),
            pltpu.VMEM((4, 32, 128), BF16),
            pltpu.VMEM((4, 32, 128), BF16),
            pltpu.VMEM((4, 8, 128), F32),
            pltpu.VMEM((8, 16, 128), BF16),
            pltpu.VMEM((2, 32, 2, 16, 128), BF16),
            pltpu.VMEM((8, 8, 128), F32),
            pltpu.VMEM((64, 1024), BF16),
            pltpu.VMEM((2, 512, 128), F32),
            pltpu.VMEM((2, 512, 128), F32),
            pltpu.VMEM((2, 512, 128), BF16),
            pltpu.VMEM((2, 512, 128), BF16),
            pltpu.VMEM((2, 32, 16, 128), BF16),
            pltpu.VMEM((64, 16, 128), BF16),
            pltpu.VMEM((128, 128), F32),
            pltpu.SemaphoreType.DMA((10,)),
            pltpu.SemaphoreType.DMA((2, 4)),
            pltpu.SemaphoreType.DMA((3,)),
            pltpu.SemaphoreType.DMA((7,)),
            pltpu.SemaphoreType.DMA((7,)),
            pltpu.SemaphoreType.DMA((4,)),
            pltpu.SemaphoreType.DMA((4,)),
            pltpu.SemaphoreType.DMA((4,)),
            pltpu.SemaphoreType.DMA((2,)),
            pltpu.SemaphoreType.DMA((2,)),
        ],
        compiler_params=pltpu.CompilerParams(
            collective_id=0, has_side_effects=True, vmem_limit_bytes=67043328
        ),
        name="layer",
    )(
        expert_ids.T,
        gate_weights.T,
        lengths,
        residual,
        query,
        fresh_token_keys,
        value_new,
        pages,
        gain,
        key_cache.reshape(4, 2, 128, PAGE, 128),
        value_cache.reshape(4, 2, 128, PAGE, 128),
        w_out,
        jnp.swapaxes(w_in, 2, 3),
        w_down,
    )


def solution(mesh):
    in_specs = (
        P("dp", "head"),
        P("dp", "head", None),
        P("dp", "head", None),
        P("dp", "head", None),
        P("dp", "head", None, None),
        P("dp", "head", None, None),
        P("dp"),
        P("dp", "head", None),
        P("head", "dp"),
        P("head"),
        P("dp", None),
        P("dp", None),
        P("dp", None, None, "head"),
        P("dp", "head", None),
    )
    out_specs = P("dp", "head")
    return jax.shard_map(shards, mesh=mesh, in_specs=in_specs, out_specs=out_specs, check_vma=False)
```

```python
import functools

import jax
import jax.numpy as jnp
from jax import lax
from jax.experimental import pallas as pl
from jax.experimental.pallas import tpu as pltpu
from jax.sharding import PartitionSpec as P

EXPERTS = 8
PAGE = 16
EPSILON = 1e-05
F32 = jnp.float32
BF16 = jnp.bfloat16
I32 = jnp.int32
MESH = pl.DeviceIdType.MESH
FAR = sorted(range(1, 32), key=lambda i: -(2 * (i >> 4) + (0, 1, 2, 1)[i >> 2 & 3] + (0, 1, 2, 1)[i & 3]))
ORDER = (0, 1, 2, 3)
SEND_B = sorted(FAR + [0], key=lambda i: i >> 3)
OUT_SPACE = pl.ANY


def whole_wait(ref, sem):
    pltpu.make_async_copy(ref, ref, sem).wait()


def layer(
    ids_hbm,
    gates_hbm,
    len_hbm,
    residual_hbm,
    query_hbm,
    fresh_hbm,
    vnew_hbm,
    pages_hbm,
    gain_hbm,
    key_hbm,
    value_hbm,
    wout_hbm,
    win_hbm,
    wdown_hbm,
    out_hbm,
    ids_ref,
    gates_ref,
    len_ref,
    page_list,
    residual_ref,
    query_ref,
    fresh_ref,
    vnew_ref,
    pages_ref,
    gain_ref,
    out_ref,
    key0,
    key1,
    key2,
    key3,
    value0,
    value1,
    value2,
    value3,
    wout_buf,
    win_buf,
    turned,
    wdown_buf,
    attn_buf,
    recv_a,
    rows_f,
    msg_buf,
    recv_m,
    recv_g,
    part_buf,
    recv_r,
    stream_buf,
    sel_buf,
    recv_b,
    recv_s,
    x_buf,
    slab_f,
    own_f,
    sib_buf,
    recv_d,
    slab_b,
    recv_c,
    mix_f,
    in_sem,
    kv_sem,
    w_sem,
    send_sem,
    recv_sem,
    group_sem,
    pass_send,
    pass_recv,
    sib_send,
    sib_recv,
):
    d = lax.axis_index("dp")
    h = lax.axis_index("head")
    y = h >> 1
    c = h & 1
    sibling = (d, h ^ 1)
    quarter = d >> 3
    block = d & 7

    barrier = pltpu.get_barrier_semaphore()

    def greet(to):
        pl.semaphore_signal(barrier, inc=1, device_id=to, device_id_type=MESH)

    small = [
        (ids_hbm, ids_ref),
        (gates_hbm, gates_ref),
        (len_hbm, len_ref),
        (pages_hbm, page_list),
        (pages_hbm, pages_ref),
        (query_hbm, query_ref),
        (fresh_hbm, fresh_ref),
        (residual_hbm, residual_ref),
        (vnew_hbm, vnew_ref),
        (gain_hbm, gain_ref),
    ]
    for n, (source, target) in enumerate(small):
        pltpu.make_async_copy(source, target, in_sem.at[n]).start()

    keys = [key0, key1, key2, key3]
    values = [value0, value1, value2, value3]

    def load_keys(b):
        return pltpu.make_async_copy(key_hbm.at[b], keys[b], kv_sem.at[0, b])

    def load_values(b):
        return pltpu.make_async_copy(value_hbm.at[b], values[b], kv_sem.at[1, b])

    load_keys(0).start()
    load_keys(1).start()

    for i in FAR:
        for side in range(2):
            greet((d ^ i, side * 2 + c))
    for i in range(1, 4):
        greet((d, h ^ i))
    for j in range(8):

        @pl.when(jnp.logical_not((h * 8 + j == d) & (quarter == h)))
        def _():
            greet((h * 8 + j, quarter))

    for b in range(2, 4):
        load_keys(b).start()
    for b in range(4):
        load_values(b).start()
    for n, (source, target) in enumerate(small):
        pltpu.make_async_copy(source, target, in_sem.at[n]).wait()

    ids = [ids_ref[j, t] for t in range(4) for j in range(2)]
    slots = []
    for a in range(8):
        earlier = jnp.int32(0)
        for n in range(a):
            earlier = earlier + (ids[n] == ids[a]).astype(I32)
        slots.append(earlier)
    lane = lax.broadcasted_iota(I32, (8, 128), 1)
    row8 = lax.broadcasted_iota(I32, (8, 128), 0)
    target = jnp.zeros((8, 128), I32)
    for t in range(4):
        for j in range(2):
            a = t * 2 + j
            value = ids[a] * 16 + block * 2 + slots[a]
            target = jnp.where((row8 == 4 + j) & (lane == block * 4 + t), value, target)
    target = target.astype(F32)
    for j in range(8):
        res = residual_ref[:, j * 128 : (j + 1) * 128].astype(F32)
        both = jnp.concatenate([res, jnp.zeros((4, 128), F32)], axis=0)
        msg_buf[j] = (both + target).astype(BF16)

    top_rows = lax.broadcasted_iota(I32, (8, 1), 0) < 4
    numbers = jnp.concatenate(
        [jnp.where(top_rows, pages_ref[b, 0:1, :], pages_ref[b, 1:2, :]) for b in range(4)],
        axis=0,
    )
    spread = (
        (lax.broadcasted_iota(I32, (64, 1024), 1) >> 4)
        == lax.broadcasted_iota(I32, (64, 1024), 0)
    ).astype(F32)
    start = jnp.dot(
        numbers.astype(F32).astype(BF16), spread.astype(BF16), preferred_element_type=F32
    )
    position = start.astype(I32) * PAGE + (lax.broadcasted_iota(I32, (32, 1024), 1) & 15)

    scale = 128.0 ** (-0.5)
    nt = (((1,), (1,)), ((), ()))

    def selected(buf, b, k):
        return jnp.concatenate([buf[k, page_list[b, k, n]] for n in range(64)], axis=0)

    def both(ref, b):
        return jnp.where(top_rows, ref[b, 0:1, :].astype(F32), ref[b, 1:2, :].astype(F32))

    def attend(pair):
        rows = jnp.concatenate([query_ref[b] for b in pair], axis=0).astype(F32)
        fresh = jnp.concatenate([both(fresh_ref, b) for b in pair], axis=0)
        own = jnp.sum(rows * fresh, axis=1, keepdims=True) * scale
        live = jnp.concatenate(
            [position[b * 8 : (b + 1) * 8] < len_ref[b] for b in pair], axis=0
        )
        scores = []
        for b in pair:
            load_keys(b).wait()
            q = query_ref[b]
            s0 = lax.dot_general(q, selected(keys[b], b, 0), nt, preferred_element_type=F32)
            s1 = lax.dot_general(q, selected(keys[b], b, 1), nt, preferred_element_type=F32)
            scores.append(jnp.where(top_rows, s0, s1))
        scores = jnp.concatenate(scores, axis=0) * scale
        masked = jnp.where(live, scores, -1e30)
        top = jnp.maximum(jnp.max(masked, axis=1, keepdims=True), own)
        expo = jnp.where(live, jnp.exp(scores - top), 0.0)
        own_expo = jnp.exp(own - top)
        total = jnp.sum(expo, axis=1, keepdims=True) + own_expo
        weights = expo / total
        own_weight = (own_expo / total).astype(BF16).astype(F32)
        for n, b in enumerate(pair):
            load_values(b).wait()
            w = weights[n * 8 : (n + 1) * 8].astype(BF16)
            a0 = jnp.dot(w, selected(values[b], b, 0), preferred_element_type=F32)
            a1 = jnp.dot(w, selected(values[b], b, 1), preferred_element_type=F32)
            new = own_weight[n * 8 : (n + 1) * 8] * both(vnew_ref, b)
            attn_buf[n * 8 : (n + 1) * 8, :] = (
                jnp.where(top_rows, a0, a1) + new
            ).astype(BF16)

    def send_rows():
        for i in FAR:
            pltpu.make_async_remote_copy(
                attn_buf, recv_a.at[d], send_sem.at[0], recv_sem.at[0], (d ^ i, h), MESH
            ).start()
        pltpu.make_async_copy(attn_buf, recv_a.at[d], recv_sem.at[0]).start()

    attend(range(4))
    pltpu.make_async_copy(wout_hbm, wout_buf, w_sem.at[0]).start()
    pltpu.make_async_copy(win_hbm.at[0], win_buf, w_sem.at[1]).start()
    pltpu.make_async_copy(wdown_hbm.at[0], wdown_buf, w_sem.at[2]).start()
    here = quarter == h
    pl.semaphore_wait(barrier, 73 - here.astype(I32))
    for j in range(8):
        own_place = here & (h * 8 + j == d)

        @pl.when(own_place)
        def _():
            pltpu.make_async_copy(msg_buf.at[j], recv_m.at[block], recv_sem.at[1]).start()

        @pl.when(jnp.logical_not(own_place))
        def _():
            pltpu.make_async_remote_copy(
                msg_buf.at[j],
                recv_m.at[block],
                send_sem.at[1],
                recv_sem.at[1],
                (h * 8 + j, quarter),
                MESH,
            ).start()

    send_rows()

    own_gains = recv_g.at[pl.ds(pl.multiple_of(h * 8, 8), 8)]
    for i in range(1, 4):
        pltpu.make_async_remote_copy(
            gain_ref, own_gains, send_sem.at[2], recv_sem.at[2], (d, h ^ i), MESH
        ).start()
    pltpu.make_async_copy(gain_ref, own_gains, recv_sem.at[2]).start()

    pltpu.make_async_copy(win_hbm.at[0], win_buf, w_sem.at[1]).wait()
    identity = (
        lax.broadcasted_iota(I32, (256, 256), 0) == lax.broadcasted_iota(I32, (256, 256), 1)
    ).astype(F32).astype(BF16)
    for m in range(2):
        for n in range(16):
            part = win_buf[m, :, n * 256 : (n + 1) * 256]
            turned[m, n * 256 : (n + 1) * 256, :] = lax.dot_general(
                identity, part, nt, preferred_element_type=F32
            ).astype(BF16)

    whole_wait(recv_m, recv_sem.at[1])
    messages = recv_m[...].astype(F32).reshape(64, 128).astype(BF16)
    pick_row = lax.broadcasted_iota(I32, (40, 64), 0)
    pick_col = lax.broadcasted_iota(I32, (40, 64), 1)
    pick = (
        ((pick_row < 32) & (pick_col == (pick_row >> 2) * 8 + (pick_row & 3)))
        | ((pick_row == 32) & ((pick_col & 7) == 4))
        | ((pick_row == 33) & ((pick_col & 7) == 5))
    )
    picked = jnp.dot(pick.astype(F32).astype(BF16), messages, preferred_element_type=F32)
    residual = picked[:32]
    slot_row = lax.broadcasted_iota(I32, (128, 128), 0).astype(F32)
    select = ((slot_row == picked[32:33]) | (slot_row == picked[33:34])).astype(F32)
    select = select[:, :32].astype(BF16)
    pltpu.make_async_copy(wout_hbm, wout_buf, w_sem.at[0]).wait()

    whole_wait(recv_a, recv_sem.at[0])
    rows_f[...] = recv_a[...].astype(F32).reshape(1024, 128)
    columns = jnp.zeros((128, 128), F32)
    for n in range(4):
        pair = jnp.concatenate(
            [rows_f[pl.ds(n * 2 + m, 128, stride=8), :] for m in range(2)], axis=1
        ).astype(BF16)
        columns = columns + jnp.dot(
            pair, wout_buf[n * 256 : (n + 1) * 256, :], preferred_element_type=F32
        )
    part_buf[...] = columns.astype(BF16).reshape(4, 32, 128)

    for i in (3, 2, 1):
        to = h ^ i
        pltpu.make_async_remote_copy(
            part_buf.at[to], recv_r.at[h], send_sem.at[3], recv_sem.at[3], (d, to), MESH
        ).start()
    pltpu.make_async_copy(part_buf.at[h], recv_r.at[h], recv_sem.at[3]).start()
    whole_wait(recv_r, recv_sem.at[3])
    stream = residual
    for i in range(4):
        stream = stream + recv_r[i].astype(F32)
    stream_buf[...] = stream.reshape(4, 8, 128)
    sel_buf[...] = (
        jnp.dot(select, stream.astype(BF16), preferred_element_type=F32)
        .astype(BF16)
        .reshape(8, 16, 128)
    )

    slot = block
    for i in SEND_B:
        to = d ^ i
        for side in range(2):
            place = recv_b.at[c, (i & 24) + slot, y]

            def remote():
                pltpu.make_async_remote_copy(
                    sel_buf.at[to >> 2],
                    place,
                    send_sem.at[4],
                    group_sem.at[i >> 3],
                    (to, side * 2 + c),
                    MESH,
                ).start()

            if i:
                remote()
            else:
                pl.when(y != side)(remote)
    pltpu.make_async_copy(sel_buf.at[d >> 2], recv_b.at[c, slot, y], group_sem.at[0]).start()

    for b in range(8):
        own_place = here & (h * 8 + b == d)

        @pl.when(own_place)
        def _():
            pltpu.make_async_copy(
                stream_buf.at[b // 2], recv_s.at[block], recv_sem.at[5]
            ).start()

        @pl.when(jnp.logical_not(own_place))
        def _():
            pltpu.make_async_remote_copy(
                stream_buf.at[b // 2],
                recv_s.at[block],
                send_sem.at[5],
                recv_sem.at[5],
                (h * 8 + b, quarter),
                MESH,
            ).start()

    pltpu.make_async_copy(wdown_hbm.at[0], wdown_buf, w_sem.at[2]).wait()
    whole_wait(recv_g, recv_sem.at[2])

    def hand_on(k):
        return pltpu.make_async_remote_copy(
            recv_b.at[c, pl.ds(k * 8, 8)],
            recv_b.at[c, pl.ds(k * 8, 8)],
            pass_send.at[k],
            pass_recv.at[k],
            sibling,
            MESH,
        )

    def arrived(k):
        whole_wait(recv_b.at[c, pl.ds(k * 8, 8)], group_sem.at[k])
        hand_on(k).start()

    squares = jnp.zeros((64, 128), F32)
    gate = jnp.zeros((64, 448), F32)
    up = jnp.zeros((64, 448), F32)
    arrived(ORDER[0])
    for n in range(4):
        k = ORDER[n]
        if n < 3:
            arrived(ORDER[n + 1])
        whole_wait(recv_b.at[1 - c, pl.ds(k * 8, 8)], pass_recv.at[k])
        first = quarter ^ k
        gains = recv_g[pl.ds(pl.multiple_of(first * 8, 8), 8), :]
        for m in range(8):
            x = recv_b[:, k * 8 + m].reshape(64, 128).astype(F32)
            squares = squares + x * x
            x_buf[:, m * 128 : (m + 1) * 128] = (x * gains[m : m + 1]).astype(BF16)
        columns = pl.ds(pl.multiple_of(first * 1024, 1024), 1024)
        x = x_buf[...]
        gate = gate + jnp.dot(x, turned[0, columns], preferred_element_type=F32)
        up = up + jnp.dot(x, turned[1, columns], preferred_element_type=F32)
    inverse = lax.rsqrt(jnp.sum(squares, axis=1, keepdims=True) * (1.0 / 4096.0) + EPSILON)
    gate = gate * inverse
    hidden = (gate * jax.nn.sigmoid(gate) * (up * inverse)).astype(BF16)

    def slab(side, core, store):
        base = (side * 2 + core) * 1024
        for n in range(4):
            columns = pl.ds(pl.multiple_of(base + n * 256, 256), 256)
            part = jnp.dot(hidden, wdown_buf[:, columns], preferred_element_type=F32)
            for m in range(2):
                store[pl.ds(n * 2 + m, 64, stride=8), :] = part[:, m * 128 : (m + 1) * 128]
        return store[...]

    def to_sibling(side):
        return pltpu.make_async_remote_copy(
            sib_buf.at[side],
            recv_d.at[side],
            sib_send.at[side],
            sib_recv.at[side],
            sibling,
            MESH,
        )

    for side in range(2):
        sib_buf[side] = slab(side, 1 - c, slab_f.at[side]).astype(BF16)
        to_sibling(side).start()
    for side in range(2):
        slab(side, c, own_f.at[side])
    for side in range(2):
        to_sibling(side).wait_recv()
        total = own_f[side] + recv_d[side].astype(F32)
        slab_b[side] = total.astype(BF16).reshape(32, 16, 128)
        for i in FAR + [0]:
            to = d ^ i
            rows = ((to >> 3) & 1) * 16 + (to >> 4) * 8 + (to & 7)

            def remote():
                pltpu.make_async_remote_copy(
                    slab_b.at[side, rows],
                    recv_c.at[d * 2 + y],
                    send_sem.at[6],
                    recv_sem.at[6],
                    (to, side * 2 + c),
                    MESH,
                ).start()

            if i:
                remote()
            else:
                pl.when(y != side)(remote)
    rows = ((d >> 3) & 1) * 16 + (d >> 4) * 8 + (d & 7)
    pltpu.make_async_copy(slab_b.at[y, rows], recv_c.at[d * 2 + y], recv_sem.at[6]).start()

    slot16 = lax.broadcasted_iota(I32, (16, 128), 0)
    factors = []
    for t in range(4):
        factor = jnp.zeros((16, 128), F32)
        for j in range(2):
            a = t * 2 + j
            factor = factor + jnp.where(slot16 == ids[a] * 2 + slots[a], gates_ref[j, t], 0.0)
        factors.append(factor)
    odd = (d & 1) == 1

    whole_wait(recv_s, recv_sem.at[5])
    whole_wait(recv_c, recv_sem.at[6])
    for e in range(8):
        total = recv_c[e * 8].astype(F32)
        for i in range(1, 8):
            total = total + recv_c[e * 8 + i].astype(F32)
        mix_f[e * 16 : (e + 1) * 16, :] = total
    for j in range(8):
        slot_rows = mix_f[pl.ds(j, 16, stride=8), :]
        mixed = jnp.concatenate(
            [jnp.sum(slot_rows * f, axis=0, keepdims=True) for f in factors], axis=0
        )
        own_stream = recv_s[j]
        own_stream = jnp.where(odd, own_stream[4:], own_stream[:4])
        out_ref[:, j * 128 : (j + 1) * 128] = (own_stream + mixed).astype(BF16)

    result = pltpu.make_async_copy(out_ref, out_hbm, w_sem.at[0])
    result.start()
    whole_wait(recv_a.at[pl.ds(0, 31)], send_sem.at[0])

    @pl.when(here)
    def _():
        whole_wait(recv_m.at[pl.ds(0, 7)], send_sem.at[1])
        whole_wait(recv_s.at[pl.ds(0, 7)], send_sem.at[5])

    @pl.when(jnp.logical_not(here))
    def _():
        whole_wait(recv_m, send_sem.at[1])
        whole_wait(recv_s, send_sem.at[5])

    whole_wait(recv_g.at[pl.ds(0, 24)], send_sem.at[2])
    whole_wait(recv_r.at[pl.ds(0, 3)], send_sem.at[3])
    whole_wait(recv_c.at[pl.ds(0, 63)], send_sem.at[4])
    whole_wait(recv_c.at[pl.ds(0, 63)], send_sem.at[6])
    for k in range(4):
        hand_on(k).wait_send()
    for side in range(2):
        to_sibling(side).wait_send()
    result.wait()


def shards(
    residual,
    query,
    fresh_token_keys,
    value_new,
    key_cache,
    value_cache,
    lengths,
    pages,
    w_out,
    norm_gain,
    expert_ids,
    gate_weights,
    w_in,
    w_down,
):
    hbm = pl.BlockSpec(memory_space=pltpu.HBM)
    gain = norm_gain.reshape(8, 128)
    return pl.pallas_call(
        layer,
        out_shape=jax.ShapeDtypeStruct((4, 1024), BF16),
        in_specs=[hbm] * 14,
        out_specs=pl.BlockSpec(memory_space=OUT_SPACE),
        scratch_shapes=[
            pltpu.SMEM((2, 4), I32),
            pltpu.SMEM((2, 4), F32),
            pltpu.SMEM((4,), I32),
            pltpu.SMEM(pages.shape, I32),
            pltpu.VMEM(residual.shape, BF16),
            pltpu.VMEM(query.shape, BF16),
            pltpu.VMEM(fresh_token_keys.shape, BF16),
            pltpu.VMEM(value_new.shape, BF16),
            pltpu.VMEM(pages.shape, I32),
            pltpu.VMEM(gain.shape, F32),
            pltpu.VMEM((4, 1024), BF16),
        ]
        + [pltpu.VMEM((2, 128, PAGE, 128), BF16)] * 8
        + [
            pltpu.VMEM((1024, 128), BF16),
            pltpu.VMEM((2, 448, 4096), BF16),
            pltpu.VMEM((2, 4096, 448), BF16),
            pltpu.VMEM((448, 4096), BF16),
            pltpu.VMEM((32, 128), BF16),
            pltpu.VMEM((32, 32, 128), BF16),
            pltpu.VMEM((1024, 128), F32),
            pltpu.VMEM((8, 8, 128), BF16),
            pltpu.VMEM((8, 8, 128), BF16),
            pltpu.VMEM((32, 128), F32),
            pltpu.VMEM((4, 32, 128), BF16),
            pltpu.VMEM((4, 32, 128), BF16),
            pltpu.VMEM((4, 8, 128), F32),
            pltpu.VMEM((8, 16, 128), BF16),
            pltpu.VMEM((2, 32, 2, 16, 128), BF16),
            pltpu.VMEM((8, 8, 128), F32),
            pltpu.VMEM((64, 1024), BF16),
            pltpu.VMEM((2, 512, 128), F32),
            pltpu.VMEM((2, 512, 128), F32),
            pltpu.VMEM((2, 512, 128), BF16),
            pltpu.VMEM((2, 512, 128), BF16),
            pltpu.VMEM((2, 32, 16, 128), BF16),
            pltpu.VMEM((64, 16, 128), BF16),
            pltpu.VMEM((128, 128), F32),
            pltpu.SemaphoreType.DMA((10,)),
            pltpu.SemaphoreType.DMA((2, 4)),
            pltpu.SemaphoreType.DMA((3,)),
            pltpu.SemaphoreType.DMA((7,)),
            pltpu.SemaphoreType.DMA((7,)),
            pltpu.SemaphoreType.DMA((4,)),
            pltpu.SemaphoreType.DMA((4,)),
            pltpu.SemaphoreType.DMA((4,)),
            pltpu.SemaphoreType.DMA((2,)),
            pltpu.SemaphoreType.DMA((2,)),
        ],
        compiler_params=pltpu.CompilerParams(
            collective_id=0, has_side_effects=True, vmem_limit_bytes=67043328
        ),
        name="layer",
    )(
        expert_ids.T,
        gate_weights.T,
        lengths,
        residual,
        query,
        fresh_token_keys,
        value_new,
        pages,
        gain,
        key_cache.reshape(4, 2, 128, PAGE, 128),
        value_cache.reshape(4, 2, 128, PAGE, 128),
        w_out,
        jnp.swapaxes(w_in, 2, 3),
        w_down,
    )


def solution(mesh):
    in_specs = (
        P("dp", "head"),
        P("dp", "head", None),
        P("dp", "head", None),
        P("dp", "head", None),
        P("dp", "head", None, None),
        P("dp", "head", None, None),
        P("dp"),
        P("dp", "head", None),
        P("head", "dp"),
        P("head"),
        P("dp", None),
        P("dp", None),
        P("dp", None, None, "head"),
        P("dp", "head", None),
    )
    out_specs = P("dp", "head")
    return jax.shard_map(shards, mesh=mesh, in_specs=in_specs, out_specs=out_specs, check_vma=False)
```

```python
import functools

import jax
import jax.numpy as jnp
from jax import lax
from jax.experimental import pallas as pl
from jax.experimental.pallas import tpu as pltpu
from jax.sharding import PartitionSpec as P

EXPERTS = 8
PAGE = 16
EPSILON = 1e-05
F32 = jnp.float32
BF16 = jnp.bfloat16
I32 = jnp.int32
MESH = pl.DeviceIdType.MESH
FAR = sorted(range(1, 32), key=lambda i: -(2 * (i >> 4) + (0, 1, 2, 1)[i >> 2 & 3] + (0, 1, 2, 1)[i & 3]))
ORDER = (0, 1, 2, 3)
SEND_B = sorted(FAR + [0], key=lambda i: i >> 3)
OUT_SPACE = pl.ANY


def whole_wait(ref, sem):
    pltpu.make_async_copy(ref, ref, sem).wait()


def layer(
    ids_hbm,
    gates_hbm,
    len_hbm,
    residual_hbm,
    query_hbm,
    fresh_hbm,
    vnew_hbm,
    pages_hbm,
    gain_hbm,
    key_hbm,
    value_hbm,
    wout_hbm,
    win_hbm,
    wdown_hbm,
    out_hbm,
    ids_ref,
    gates_ref,
    len_ref,
    page_list,
    residual_ref,
    query_ref,
    fresh_ref,
    vnew_ref,
    pages_ref,
    gain_ref,
    out_ref,
    key0,
    key1,
    key2,
    key3,
    value0,
    value1,
    value2,
    value3,
    wout_buf,
    win_buf,
    turned,
    wdown_buf,
    attn_buf,
    recv_a,
    rows_f,
    msg_buf,
    recv_m,
    recv_g,
    part_buf,
    recv_r,
    stream_buf,
    sel_buf,
    recv_b,
    recv_s,
    x_buf,
    slab_f,
    own_f,
    sib_buf,
    recv_d,
    slab_b,
    recv_c,
    mix_f,
    in_sem,
    kv_sem,
    w_sem,
    send_sem,
    recv_sem,
    group_sem,
    pass_send,
    pass_recv,
    sib_send,
    sib_recv,
):
    d = lax.axis_index("dp")
    h = lax.axis_index("head")
    y = h >> 1
    c = h & 1
    sibling = (d, h ^ 1)
    quarter = d >> 3
    block = d & 7

    barrier = pltpu.get_barrier_semaphore()

    def greet(to):
        pl.semaphore_signal(barrier, inc=1, device_id=to, device_id_type=MESH)

    small = [
        (ids_hbm, ids_ref),
        (gates_hbm, gates_ref),
        (len_hbm, len_ref),
        (pages_hbm, page_list),
        (pages_hbm, pages_ref),
        (query_hbm, query_ref),
        (fresh_hbm, fresh_ref),
        (residual_hbm, residual_ref),
        (vnew_hbm, vnew_ref),
        (gain_hbm, gain_ref),
    ]
    for n, (source, target) in enumerate(small):
        pltpu.make_async_copy(source, target, in_sem.at[n]).start()

    keys = [key0, key1, key2, key3]
    values = [value0, value1, value2, value3]

    def load_keys(b):
        return pltpu.make_async_copy(key_hbm.at[b], keys[b], kv_sem.at[0, b])

    def load_values(b):
        return pltpu.make_async_copy(value_hbm.at[b], values[b], kv_sem.at[1, b])

    load_keys(0).start()
    load_keys(1).start()

    for i in FAR:
        for side in range(2):
            greet((d ^ i, side * 2 + c))
    for i in range(1, 4):
        greet((d, h ^ i))
    for j in range(8):

        @pl.when(jnp.logical_not((h * 8 + j == d) & (quarter == h)))
        def _():
            greet((h * 8 + j, quarter))

    for b in range(2, 4):
        load_keys(b).start()
    for b in range(4):
        load_values(b).start()
    for n, (source, target) in enumerate(small):
        pltpu.make_async_copy(source, target, in_sem.at[n]).wait()

    ids = [ids_ref[j, t] for t in range(4) for j in range(2)]
    slots = []
    for a in range(8):
        earlier = jnp.int32(0)
        for n in range(a):
            earlier = earlier + (ids[n] == ids[a]).astype(I32)
        slots.append(earlier)
    lane = lax.broadcasted_iota(I32, (8, 128), 1)
    row8 = lax.broadcasted_iota(I32, (8, 128), 0)
    target = jnp.zeros((8, 128), I32)
    for t in range(4):
        for j in range(2):
            a = t * 2 + j
            value = ids[a] * 16 + block * 2 + slots[a]
            target = jnp.where((row8 == 4 + j) & (lane == block * 4 + t), value, target)
    target = target.astype(F32)
    for j in range(8):
        res = residual_ref[:, j * 128 : (j + 1) * 128].astype(F32)
        both = jnp.concatenate([res, jnp.zeros((4, 128), F32)], axis=0)
        msg_buf[j] = (both + target).astype(BF16)

    top_rows = lax.broadcasted_iota(I32, (8, 1), 0) < 4
    numbers = jnp.concatenate(
        [jnp.where(top_rows, pages_ref[b, 0:1, :], pages_ref[b, 1:2, :]) for b in range(4)],
        axis=0,
    )
    spread = (
        (lax.broadcasted_iota(I32, (64, 1024), 1) >> 4)
        == lax.broadcasted_iota(I32, (64, 1024), 0)
    ).astype(F32)
    start = jnp.dot(
        numbers.astype(F32).astype(BF16), spread.astype(BF16), preferred_element_type=F32
    )
    position = start.astype(I32) * PAGE + (lax.broadcasted_iota(I32, (32, 1024), 1) & 15)

    scale = 128.0 ** (-0.5)
    nt = (((1,), (1,)), ((), ()))

    def selected(buf, b, k):
        return jnp.concatenate([buf[k, page_list[b, k, n]] for n in range(64)], axis=0)

    def both(ref, b):
        return jnp.where(top_rows, ref[b, 0:1, :].astype(F32), ref[b, 1:2, :].astype(F32))

    def attend(pair):
        rows = jnp.concatenate([query_ref[b] for b in pair], axis=0).astype(F32)
        fresh = jnp.concatenate([both(fresh_ref, b) for b in pair], axis=0)
        own = jnp.sum(rows * fresh, axis=1, keepdims=True) * scale
        live = jnp.concatenate(
            [position[b * 8 : (b + 1) * 8] < len_ref[b] for b in pair], axis=0
        )
        scores = []
        for b in pair:
            load_keys(b).wait()
            q = query_ref[b]
            s0 = lax.dot_general(q, selected(keys[b], b, 0), nt, preferred_element_type=F32)
            s1 = lax.dot_general(q, selected(keys[b], b, 1), nt, preferred_element_type=F32)
            scores.append(jnp.where(top_rows, s0, s1))
        scores = jnp.concatenate(scores, axis=0) * scale
        masked = jnp.where(live, scores, -1e30)
        top = jnp.maximum(jnp.max(masked, axis=1, keepdims=True), own)
        expo = jnp.where(live, jnp.exp(scores - top), 0.0)
        own_expo = jnp.exp(own - top)
        total = jnp.sum(expo, axis=1, keepdims=True) + own_expo
        weights = expo / total
        own_weight = (own_expo / total).astype(BF16).astype(F32)
        for n, b in enumerate(pair):
            load_values(b).wait()
            w = weights[n * 8 : (n + 1) * 8].astype(BF16)
            a0 = jnp.dot(w, selected(values[b], b, 0), preferred_element_type=F32)
            a1 = jnp.dot(w, selected(values[b], b, 1), preferred_element_type=F32)
            new = own_weight[n * 8 : (n + 1) * 8] * both(vnew_ref, b)
            attn_buf[n * 8 : (n + 1) * 8, :] = (
                jnp.where(top_rows, a0, a1) + new
            ).astype(BF16)

    def send_rows():
        for i in FAR:
            pltpu.make_async_remote_copy(
                attn_buf, recv_a.at[d], send_sem.at[0], recv_sem.at[0], (d ^ i, h), MESH
            ).start()
        pltpu.make_async_copy(attn_buf, recv_a.at[d], recv_sem.at[0]).start()

    attend(range(4))
    pltpu.make_async_copy(wout_hbm, wout_buf, w_sem.at[0]).start()
    pltpu.make_async_copy(win_hbm.at[0], win_buf, w_sem.at[1]).start()
    pltpu.make_async_copy(wdown_hbm.at[0], wdown_buf, w_sem.at[2]).start()
    here = quarter == h
    pl.semaphore_wait(barrier, 73 - here.astype(I32))
    for j in range(8):
        own_place = here & (h * 8 + j == d)

        @pl.when(own_place)
        def _():
            pltpu.make_async_copy(msg_buf.at[j], recv_m.at[block], recv_sem.at[1]).start()

        @pl.when(jnp.logical_not(own_place))
        def _():
            pltpu.make_async_remote_copy(
                msg_buf.at[j],
                recv_m.at[block],
                send_sem.at[1],
                recv_sem.at[1],
                (h * 8 + j, quarter),
                MESH,
            ).start()

    send_rows()

    own_gains = recv_g.at[pl.ds(pl.multiple_of(h * 8, 8), 8)]
    for i in range(1, 4):
        pltpu.make_async_remote_copy(
            gain_ref, own_gains, send_sem.at[2], recv_sem.at[2], (d, h ^ i), MESH
        ).start()
    pltpu.make_async_copy(gain_ref, own_gains, recv_sem.at[2]).start()

    pltpu.make_async_copy(win_hbm.at[0], win_buf, w_sem.at[1]).wait()
    identity = (
        lax.broadcasted_iota(I32, (256, 256), 0) == lax.broadcasted_iota(I32, (256, 256), 1)
    ).astype(F32).astype(BF16)

    def turn(m):
        for n in range(16):
            part = win_buf[m, :, n * 256 : (n + 1) * 256]
            turned[m, n * 256 : (n + 1) * 256, :] = lax.dot_general(
                identity, part, nt, preferred_element_type=F32
            ).astype(BF16)

    turn(0)

    whole_wait(recv_m, recv_sem.at[1])
    messages = recv_m[...].astype(F32).reshape(64, 128).astype(BF16)
    pick_row = lax.broadcasted_iota(I32, (40, 64), 0)
    pick_col = lax.broadcasted_iota(I32, (40, 64), 1)
    pick = (
        ((pick_row < 32) & (pick_col == (pick_row >> 2) * 8 + (pick_row & 3)))
        | ((pick_row == 32) & ((pick_col & 7) == 4))
        | ((pick_row == 33) & ((pick_col & 7) == 5))
    )
    picked = jnp.dot(pick.astype(F32).astype(BF16), messages, preferred_element_type=F32)
    residual = picked[:32]
    slot_row = lax.broadcasted_iota(I32, (128, 128), 0).astype(F32)
    select = ((slot_row == picked[32:33]) | (slot_row == picked[33:34])).astype(F32)
    select = select[:, :32].astype(BF16)
    pltpu.make_async_copy(wout_hbm, wout_buf, w_sem.at[0]).wait()

    whole_wait(recv_a, recv_sem.at[0])
    rows_f[...] = recv_a[...].astype(F32).reshape(1024, 128)
    columns = jnp.zeros((128, 128), F32)
    for n in range(4):
        pair = jnp.concatenate(
            [rows_f[pl.ds(n * 2 + m, 128, stride=8), :] for m in range(2)], axis=1
        ).astype(BF16)
        columns = columns + jnp.dot(
            pair, wout_buf[n * 256 : (n + 1) * 256, :], preferred_element_type=F32
        )
    part_buf[...] = columns.astype(BF16).reshape(4, 32, 128)

    for i in (3, 2, 1):
        to = h ^ i
        pltpu.make_async_remote_copy(
            part_buf.at[to], recv_r.at[h], send_sem.at[3], recv_sem.at[3], (d, to), MESH
        ).start()
    pltpu.make_async_copy(part_buf.at[h], recv_r.at[h], recv_sem.at[3]).start()
    turn(1)
    whole_wait(recv_r, recv_sem.at[3])
    stream = residual
    for i in range(4):
        stream = stream + recv_r[i].astype(F32)
    stream_buf[...] = stream.reshape(4, 8, 128)
    sel_buf[...] = (
        jnp.dot(select, stream.astype(BF16), preferred_element_type=F32)
        .astype(BF16)
        .reshape(8, 16, 128)
    )

    slot = block
    for i in SEND_B:
        to = d ^ i
        for side in range(2):
            place = recv_b.at[c, (i & 24) + slot, y]

            def remote():
                pltpu.make_async_remote_copy(
                    sel_buf.at[to >> 2],
                    place,
                    send_sem.at[4],
                    group_sem.at[i >> 3],
                    (to, side * 2 + c),
                    MESH,
                ).start()

            if i:
                remote()
            else:
                pl.when(y != side)(remote)
    pltpu.make_async_copy(sel_buf.at[d >> 2], recv_b.at[c, slot, y], group_sem.at[0]).start()

    for b in range(8):
        own_place = here & (h * 8 + b == d)

        @pl.when(own_place)
        def _():
            pltpu.make_async_copy(
                stream_buf.at[b // 2], recv_s.at[block], recv_sem.at[5]
            ).start()

        @pl.when(jnp.logical_not(own_place))
        def _():
            pltpu.make_async_remote_copy(
                stream_buf.at[b // 2],
                recv_s.at[block],
                send_sem.at[5],
                recv_sem.at[5],
                (h * 8 + b, quarter),
                MESH,
            ).start()

    pltpu.make_async_copy(wdown_hbm.at[0], wdown_buf, w_sem.at[2]).wait()
    whole_wait(recv_g, recv_sem.at[2])

    def hand_on(k):
        return pltpu.make_async_remote_copy(
            recv_b.at[c, pl.ds(k * 8, 8)],
            recv_b.at[c, pl.ds(k * 8, 8)],
            pass_send.at[k],
            pass_recv.at[k],
            sibling,
            MESH,
        )

    def arrived(k):
        whole_wait(recv_b.at[c, pl.ds(k * 8, 8)], group_sem.at[k])
        hand_on(k).start()

    squares = jnp.zeros((64, 128), F32)
    gate = jnp.zeros((64, 448), F32)
    up = jnp.zeros((64, 448), F32)
    arrived(ORDER[0])
    for n in range(4):
        k = ORDER[n]
        if n < 3:
            arrived(ORDER[n + 1])
        whole_wait(recv_b.at[1 - c, pl.ds(k * 8, 8)], pass_recv.at[k])
        first = quarter ^ k
        gains = recv_g[pl.ds(pl.multiple_of(first * 8, 8), 8), :]
        for m in range(8):
            x = recv_b[:, k * 8 + m].reshape(64, 128).astype(F32)
            squares = squares + x * x
            x_buf[:, m * 128 : (m + 1) * 128] = (x * gains[m : m + 1]).astype(BF16)
        columns = pl.ds(pl.multiple_of(first * 1024, 1024), 1024)
        x = x_buf[...]
        gate = gate + jnp.dot(x, turned[0, columns], preferred_element_type=F32)
        up = up + jnp.dot(x, turned[1, columns], preferred_element_type=F32)
    inverse = lax.rsqrt(jnp.sum(squares, axis=1, keepdims=True) * (1.0 / 4096.0) + EPSILON)
    gate = gate * inverse
    hidden = (gate * jax.nn.sigmoid(gate) * (up * inverse)).astype(BF16)

    def slab(side, core, store):
        base = (side * 2 + core) * 1024
        for n in range(4):
            columns = pl.ds(pl.multiple_of(base + n * 256, 256), 256)
            part = jnp.dot(hidden, wdown_buf[:, columns], preferred_element_type=F32)
            for m in range(2):
                store[pl.ds(n * 2 + m, 64, stride=8), :] = part[:, m * 128 : (m + 1) * 128]
        return store[...]

    def to_sibling(side):
        return pltpu.make_async_remote_copy(
            sib_buf.at[side],
            recv_d.at[side],
            sib_send.at[side],
            sib_recv.at[side],
            sibling,
            MESH,
        )

    for side in range(2):
        sib_buf[side] = slab(side, 1 - c, slab_f.at[side]).astype(BF16)
        to_sibling(side).start()
    for side in range(2):
        slab(side, c, own_f.at[side])
    for side in range(2):
        to_sibling(side).wait_recv()
        total = own_f[side] + recv_d[side].astype(F32)
        slab_b[side] = total.astype(BF16).reshape(32, 16, 128)
        for i in FAR + [0]:
            to = d ^ i
            rows = ((to >> 3) & 1) * 16 + (to >> 4) * 8 + (to & 7)

            def remote():
                pltpu.make_async_remote_copy(
                    slab_b.at[side, rows],
                    recv_c.at[d * 2 + y],
                    send_sem.at[6],
                    recv_sem.at[6],
                    (to, side * 2 + c),
                    MESH,
                ).start()

            if i:
                remote()
            else:
                pl.when(y != side)(remote)
    rows = ((d >> 3) & 1) * 16 + (d >> 4) * 8 + (d & 7)
    pltpu.make_async_copy(slab_b.at[y, rows], recv_c.at[d * 2 + y], recv_sem.at[6]).start()

    slot16 = lax.broadcasted_iota(I32, (16, 128), 0)
    factors = []
    for t in range(4):
        factor = jnp.zeros((16, 128), F32)
        for j in range(2):
            a = t * 2 + j
            factor = factor + jnp.where(slot16 == ids[a] * 2 + slots[a], gates_ref[j, t], 0.0)
        factors.append(factor)
    odd = (d & 1) == 1

    whole_wait(recv_s, recv_sem.at[5])
    whole_wait(recv_c, recv_sem.at[6])
    for e in range(8):
        total = recv_c[e * 8].astype(F32)
        for i in range(1, 8):
            total = total + recv_c[e * 8 + i].astype(F32)
        mix_f[e * 16 : (e + 1) * 16, :] = total
    for j in range(8):
        slot_rows = mix_f[pl.ds(j, 16, stride=8), :]
        mixed = jnp.concatenate(
            [jnp.sum(slot_rows * f, axis=0, keepdims=True) for f in factors], axis=0
        )
        own_stream = recv_s[j]
        own_stream = jnp.where(odd, own_stream[4:], own_stream[:4])
        out_ref[:, j * 128 : (j + 1) * 128] = (own_stream + mixed).astype(BF16)

    result = pltpu.make_async_copy(out_ref, out_hbm, w_sem.at[0])
    result.start()
    whole_wait(recv_a.at[pl.ds(0, 31)], send_sem.at[0])

    @pl.when(here)
    def _():
        whole_wait(recv_m.at[pl.ds(0, 7)], send_sem.at[1])
        whole_wait(recv_s.at[pl.ds(0, 7)], send_sem.at[5])

    @pl.when(jnp.logical_not(here))
    def _():
        whole_wait(recv_m, send_sem.at[1])
        whole_wait(recv_s, send_sem.at[5])

    whole_wait(recv_g.at[pl.ds(0, 24)], send_sem.at[2])
    whole_wait(recv_r.at[pl.ds(0, 3)], send_sem.at[3])
    whole_wait(recv_c.at[pl.ds(0, 63)], send_sem.at[4])
    whole_wait(recv_c.at[pl.ds(0, 63)], send_sem.at[6])
    for k in range(4):
        hand_on(k).wait_send()
    for side in range(2):
        to_sibling(side).wait_send()
    result.wait()


def shards(
    residual,
    query,
    fresh_token_keys,
    value_new,
    key_cache,
    value_cache,
    lengths,
    pages,
    w_out,
    norm_gain,
    expert_ids,
    gate_weights,
    w_in,
    w_down,
):
    hbm = pl.BlockSpec(memory_space=pltpu.HBM)
    gain = norm_gain.reshape(8, 128)
    return pl.pallas_call(
        layer,
        out_shape=jax.ShapeDtypeStruct((4, 1024), BF16),
        in_specs=[hbm] * 14,
        out_specs=pl.BlockSpec(memory_space=OUT_SPACE),
        scratch_shapes=[
            pltpu.SMEM((2, 4), I32),
            pltpu.SMEM((2, 4), F32),
            pltpu.SMEM((4,), I32),
            pltpu.SMEM(pages.shape, I32),
            pltpu.VMEM(residual.shape, BF16),
            pltpu.VMEM(query.shape, BF16),
            pltpu.VMEM(fresh_token_keys.shape, BF16),
            pltpu.VMEM(value_new.shape, BF16),
            pltpu.VMEM(pages.shape, I32),
            pltpu.VMEM(gain.shape, F32),
            pltpu.VMEM((4, 1024), BF16),
        ]
        + [pltpu.VMEM((2, 128, PAGE, 128), BF16)] * 8
        + [
            pltpu.VMEM((1024, 128), BF16),
            pltpu.VMEM((2, 448, 4096), BF16),
            pltpu.VMEM((2, 4096, 448), BF16),
            pltpu.VMEM((448, 4096), BF16),
            pltpu.VMEM((32, 128), BF16),
            pltpu.VMEM((32, 32, 128), BF16),
            pltpu.VMEM((1024, 128), F32),
            pltpu.VMEM((8, 8, 128), BF16),
            pltpu.VMEM((8, 8, 128), BF16),
            pltpu.VMEM((32, 128), F32),
            pltpu.VMEM((4, 32, 128), BF16),
            pltpu.VMEM((4, 32, 128), BF16),
            pltpu.VMEM((4, 8, 128), F32),
            pltpu.VMEM((8, 16, 128), BF16),
            pltpu.VMEM((2, 32, 2, 16, 128), BF16),
            pltpu.VMEM((8, 8, 128), F32),
            pltpu.VMEM((64, 1024), BF16),
            pltpu.VMEM((2, 512, 128), F32),
            pltpu.VMEM((2, 512, 128), F32),
            pltpu.VMEM((2, 512, 128), BF16),
            pltpu.VMEM((2, 512, 128), BF16),
            pltpu.VMEM((2, 32, 16, 128), BF16),
            pltpu.VMEM((64, 16, 128), BF16),
            pltpu.VMEM((128, 128), F32),
            pltpu.SemaphoreType.DMA((10,)),
            pltpu.SemaphoreType.DMA((2, 4)),
            pltpu.SemaphoreType.DMA((3,)),
            pltpu.SemaphoreType.DMA((7,)),
            pltpu.SemaphoreType.DMA((7,)),
            pltpu.SemaphoreType.DMA((4,)),
            pltpu.SemaphoreType.DMA((4,)),
            pltpu.SemaphoreType.DMA((4,)),
            pltpu.SemaphoreType.DMA((2,)),
            pltpu.SemaphoreType.DMA((2,)),
        ],
        compiler_params=pltpu.CompilerParams(
            collective_id=0, has_side_effects=True, vmem_limit_bytes=67043328
        ),
        name="layer",
    )(
        expert_ids.T,
        gate_weights.T,
        lengths,
        residual,
        query,
        fresh_token_keys,
        value_new,
        pages,
        gain,
        key_cache.reshape(4, 2, 128, PAGE, 128),
        value_cache.reshape(4, 2, 128, PAGE, 128),
        w_out,
        jnp.swapaxes(w_in, 2, 3),
        w_down,
    )


def solution(mesh):
    in_specs = (
        P("dp", "head"),
        P("dp", "head", None),
        P("dp", "head", None),
        P("dp", "head", None),
        P("dp", "head", None, None),
        P("dp", "head", None, None),
        P("dp"),
        P("dp", "head", None),
        P("head", "dp"),
        P("head"),
        P("dp", None),
        P("dp", None),
        P("dp", None, None, "head"),
        P("dp", "head", None),
    )
    out_specs = P("dp", "head")
    return jax.shard_map(shards, mesh=mesh, in_specs=in_specs, out_specs=out_specs, check_vma=False)
```
